32 devices in a mesh: dp: 4 (over x, core), seq: 8 (over z, y).
Axes of the slice: x: 2, y: 2, z: 4, core: 2. Of those that a mesh axis runs over, the one named last changes fastest.
Arguments:
- block_input: bfloat16 [4, 1024, 2048], P('dp', 'seq'), may hold values from -6 to 6
- norm_gain: bfloat16 [2048], P(('dp', 'seq')), may hold values from 0.5 to 1.5
- in_weight: bfloat16 [2048, 8192], P(('dp', 'seq')), may hold values from -0.125 to 0.125
- conv_weight: bfloat16 [4096, 4], P(('dp', 'seq')), may hold values from -3 to 3
- conv_bias: bfloat16 [4096], P(('dp', 'seq')), may hold values from -3 to 3
- select_weight: bfloat16 [4096, 160], P(('dp', 'seq')), may hold values from -0.09375 to 0.09375
- step_weight: bfloat16 [4096, 128], P(('dp', 'seq')), may hold values from -0.5 to 0.5
- step_bias: bfloat16 [4096], P(('dp', 'seq')), may hold values from -7 to -2.25
- decay_log: bfloat16 [4096, 16], P(('dp', 'seq')), may hold values from -3 to 2.765625
- skip_gain: bfloat16 [4096], P(('dp', 'seq')), may hold values from 0.5 to 1.5
- out_weight: bfloat16 [4096, 2048], P(('dp', 'seq')), may hold values from -0.1875 to 0.1875
- output_grad: bfloat16 [4, 1024, 2048], P('dp', 'seq'), may hold values from -6 to 6
Outputs:
- layer_output: bfloat16 [4, 1024, 2048], P('dp', 'seq')
- input_grad: bfloat16 [4, 1024, 2048], P('dp', 'seq')
- grad_norm_gain: float32 [2048], P(('dp', 'seq'))
- grad_in_weight: float32 [2048, 8192], P(('dp', 'seq'))
- grad_conv_weight: float32 [4096, 4], P(('dp', 'seq'))
- grad_conv_bias: float32 [4096], P(('dp', 'seq'))
- grad_select_weight: float32 [4096, 160], P(('dp', 'seq'))
- grad_step_weight: float32 [4096, 128], P(('dp', 'seq'))
- grad_step_bias: float32 [4096], P(('dp', 'seq'))
- grad_decay_log: float32 [4096, 16], P(('dp', 'seq'))
- grad_skip_gain: float32 [4096], P(('dp', 'seq'))
- grad_out_weight: float32 [4096, 2048], P(('dp', 'seq'))
The draws below stay inside these ranges and needn't reach their ends.
All inputs are finite; a program needn't handle non-finite values.
Results may differ from the reference program's by a relative error of at most 0.012.
Values may be sent and summed in bfloat16 or wider, within the bound.
A program may use at most 320 MiB of HBM per device.

```python
import jax
import jax.numpy as jnp
from jax import lax

D = 2048
E = 4096
STATE = 16
RANK = 128
KERNEL = 4
LENGTH = 1024
BATCH = 4


def steps_of(rng, dims, split, least, top_value):
    def one(axis_at, parts):
        steps = jax.random.uniform(jax.random.fold_in(jax.random.fold_in(rng, 6), axis_at), (parts,), jnp.float32, least / len(split), top_value / len(split))
        return jnp.repeat(jnp.exp(steps), dims[axis_at] // parts).reshape((-1,) + (1,) * (len(dims) - axis_at - 1))

    gain = one(*split[0])
    for cut in split[1:]:
        gain = gain * one(*cut)
    return gain


def normal_values(stream_key, dims, width, most, cuts=(), dtype=jnp.bfloat16):
    drawn = width * jax.random.normal(stream_key, dims, jnp.float32)
    if cuts:
        drawn = drawn * steps_of(stream_key, dims, cuts, -0.22, 0.18)
    return jnp.clip(drawn, -most, most).astype(dtype)


def setup_inputs(seed: int = 0) -> dict:
    arg_keys = jax.random.split(jax.random.key(seed), 13)
    block_input = normal_values(arg_keys[0], (BATCH, LENGTH, D), 1.0, 6.0, ((0, 4), (1, 8)))
    norm_gain = jnp.clip(1.0 + 0.1 * jax.random.normal(arg_keys[1], (D,), jnp.float32), 0.5, 1.5).astype(jnp.bfloat16)
    in_weight = normal_values(arg_keys[2], (D, 2 * E), D ** -0.5, 0.125, ((0, 32),))
    conv_weight = normal_values(arg_keys[3], (E, KERNEL), KERNEL ** -0.5, 3.0, ((0, 32),))
    conv_bias = normal_values(arg_keys[4], (E,), 0.5, 3.0, ((0, 32),))
    select_weight = normal_values(arg_keys[5], (E, RANK + 2 * STATE), E ** -0.5, 0.09375, ((0, 32),))
    step_weight = normal_values(arg_keys[6], (E, RANK), RANK ** -0.5, 0.5, ((0, 32),))
    step_bias = jnp.clip(-7.0 + 4.75 * jax.random.uniform(arg_keys[7], (E,), jnp.float32) ** steps_of(arg_keys[7], (E,), ((0, 32),), -0.2, 0.2), -7.0, -2.25).astype(jnp.bfloat16)
    decay_log = jnp.clip(-3.0 + 5.765625 * jax.random.uniform(arg_keys[8], (E, STATE), jnp.float32) ** steps_of(arg_keys[8], (E, STATE), ((0, 32),), -0.2, 0.2), -3.0, 2.765625).astype(jnp.bfloat16)
    skip_gain = jnp.clip(0.5 + 1.0 * jax.random.uniform(arg_keys[9], (E,), jnp.float32) ** steps_of(arg_keys[9], (E,), ((0, 32),), -0.2, 0.2), 0.5, 1.5).astype(jnp.bfloat16)
    out_weight = normal_values(arg_keys[10], (E, D), (E // 4) ** -0.5, 0.1875, ((0, 32),))
    output_grad = normal_values(arg_keys[11], (BATCH, LENGTH, D), 1.0, 6.0, ((0, 4), (1, 8)))
    return dict(block_input=block_input, norm_gain=norm_gain, in_weight=in_weight, conv_weight=conv_weight, conv_bias=conv_bias, select_weight=select_weight, step_weight=step_weight, step_bias=step_bias, decay_log=decay_log, skip_gain=skip_gain, out_weight=out_weight, output_grad=output_grad)


EPS = 1e-05
HIGH = lax.Precision.HIGHEST

@jax.custom_vjp
def low(v):
    return lax.optimization_barrier(v.astype(jnp.bfloat16)).astype(jnp.float32)

@jax.custom_vjp
def low_back(v):
    return v

def low_keep(v):
    return (low(v), None)

def low_pass(kept, grad):
    return (grad,)

def back_keep(v):
    return (v, None)

def back_low(kept, grad):
    return (low(grad),)
low.defvjp(low_keep, low_pass)
low_back.defvjp(back_keep, back_low)

def selective(inner_act, step_size, write_vec, read_vec, decay_rate):
    length = inner_act.shape[0]
    blocks = length // 64

    def one_block(carry_state, pieces):

        def one_step(state_now, token_in):
            inner_now, delta_now, write_now, read_now = token_in
            state_now = jnp.exp(delta_now[None, :] * decay_rate) * state_now + write_now[:, None] * (delta_now * inner_now)[None, :]
            return (state_now, lax.optimization_barrier(jnp.sum(state_now * read_now[:, None], axis=0)))
        return lax.scan(one_step, carry_state, pieces)
    pieces = tuple((p_arr.reshape(blocks, 64, p_arr.shape[1]) for p_arr in (inner_act, step_size, write_vec, read_vec)))
    start_state = jnp.zeros((STATE, E), jnp.float32)
    _, scanned = lax.scan(jax.checkpoint(one_block), start_state, pieces)
    return scanned.reshape(length, E)

def layer(token_rows, norm_gain, in_weight, conv_weight, conv_bias, select_weight, step_weight, step_bias, decay_log, skip_gain, out_weight):
    length = token_rows.shape[0]
    mean_sq = lax.optimization_barrier(jnp.mean(token_rows * token_rows, axis=1, keepdims=True))
    normed = low(token_rows * lax.rsqrt(mean_sq + EPS) * norm_gain)
    mixed = low_back(low(jnp.dot(normed, in_weight, precision=HIGH)))
    conv_in = mixed[:, :E]
    gate_in = mixed[:, E:]
    padded = jnp.concatenate([jnp.zeros((KERNEL - 1, E), jnp.float32), conv_in], axis=0)
    conv_out = conv_bias + jnp.zeros((length, E), jnp.float32)
    for offset in range(KERNEL):
        conv_out = conv_out + padded[offset:offset + length] * conv_weight[:, offset]
    inner_act = low(jax.nn.silu(conv_out))
    picked = low_back(low(jnp.dot(inner_act, select_weight, precision=HIGH)))
    step_in = picked[:, :RANK]
    write_vec = picked[:, RANK:RANK + STATE]
    read_vec = picked[:, RANK + STATE:]
    step_raw = low_back(jnp.dot(step_in, step_weight.T, precision=HIGH))
    step_size = jax.nn.softplus(step_raw + step_bias)
    decay_rate = -jnp.exp(decay_log.T)
    scanned = selective(inner_act, step_size, write_vec, read_vec, decay_rate)
    mamba_out = scanned + skip_gain * inner_act
    gated_out = low(mamba_out * jax.nn.silu(gate_in))
    return token_rows + jnp.dot(gated_out, out_weight, precision=HIGH)

def reference(block_input, norm_gain, in_weight, conv_weight, conv_bias, select_weight, step_weight, step_bias, decay_log, skip_gain, out_weight, output_grad):
    params = tuple((w_arr.astype(jnp.float32) for w_arr in (norm_gain, in_weight, conv_weight, conv_bias, select_weight, step_weight, step_bias, decay_log, skip_gain, out_weight)))

    def one_seq(totals, pair_in):
        seq_rows, seq_grad = pair_in
        result, pullback = jax.vjp(layer, seq_rows.astype(jnp.float32), *params)
        seq_grads = pullback(seq_grad.astype(jnp.float32))
        summed = tuple((a_arr + b_arr for a_arr, b_arr in zip(totals, seq_grads[1:])))
        return (summed, (result.astype(jnp.bfloat16), seq_grads[0].astype(jnp.bfloat16)))
    zero_grads = tuple((jnp.zeros(p_arr.shape, jnp.float32) for p_arr in params))
    totals, (layer_outs, input_grads) = lax.scan(one_seq, zero_grads, (block_input, output_grad))
    return (layer_outs, input_grads, totals[0], totals[1], totals[2], totals[3], totals[4], totals[5], totals[6], totals[7], totals[8], totals[9])
```

```python
import functools
import jax
import jax.numpy as jnp
from jax import lax
from jax.experimental import pallas as pl
from jax.experimental.pallas import tpu as pltpu
from jax.sharding import PartitionSpec as P

RANK = 128
KERNEL = 4
MESH = pl.DeviceIdType.MESH

CH = 8
NG = 8


def _expand(dst, pick_ref, base, first, chunk):
    cols = pick_ref.shape[0]
    width = NG * 128
    k_at = lax.broadcasted_iota(jnp.int32, (cols, width), 0)
    n_at = lax.broadcasted_iota(jnp.int32, (cols, width), 1) // 128
    pick_one = jnp.where(k_at == base + first + n_at, 1.0, 0.0).astype(jnp.bfloat16)
    for c in range(CH):
        tokens = pick_ref[:, c * chunk : (c + 1) * chunk]
        wide = lax.dot_general(
            tokens, pick_one, (((0,), (0,)), ((), ())), preferred_element_type=jnp.float32
        )
        for n in range(NG):
            dst.at[n][pl.ds(c, chunk, stride=CH), :] = wide[:, n * 128 : (n + 1) * 128]


def _weave(dst, value, chunk):
    for q in range(dst.shape[0]):
        for c in range(CH):
            dst.at[q][pl.ds(c, chunk, stride=CH), :] = value(
                slice(c * chunk, (c + 1) * chunk), slice(q * 128, (q + 1) * 128)
            )


def _unweave(dst, src, chunk):
    for q in range(src.shape[0]):
        for c in range(CH):
            dst[c * chunk : (c + 1) * chunk, q * 128 : (q + 1) * 128] = src.at[q][
                pl.ds(c, chunk, stride=CH), :
            ]


def _rows_mask(k, up):
    row = lax.broadcasted_iota(jnp.int32, (CH, 128), 0)
    return row < CH - k if up else row >= k


def _link(p, h, up):
    for k in (1, 2, 4):
        mask = _rows_mask(k, up)
        shift = CH - k if up else k
        ps = jnp.where(mask, pltpu.roll(p, shift, 0), 1.0)
        hs = jnp.where(mask, pltpu.roll(h, shift, 0), 0.0)
        h = h + p * hs
        p = p * ps
    return p, h


def fwd_kernel(chunk, lw, rank, state, delta_ref, inner_ref, pick_ref, a2_ref, h0_ref, y_ref, hin_ref, hend_ref, wx, rx, ab, dt, ut, yt):
    el = delta_ref.shape[1]
    _weave(dt, lambda i, j: delta_ref[i, j], chunk)
    _weave(ut, lambda i, j: delta_ref[i, j] * inner_ref[i, j], chunk)
    for g in range(state // NG):
        _expand(wx, pick_ref, rank, g * NG, chunk)
        _expand(rx, pick_ref, rank + state, g * NG, chunk)
        for q in range(el // (128 * lw)):
            tile = [q * lw + l for l in range(lw)]
            lanes = [slice((q * lw + l) * 128, (q * lw + l + 1) * 128) for l in range(lw)]
            rate = [[a2_ref[g * NG + n : g * NG + n + 1, lanes[l]] for l in range(lw)] for n in range(NG)]
            zero = jnp.zeros((CH, 128), jnp.float32)

            def first(t, carry):
                h, cum = carry
                row = pl.ds(pl.multiple_of(t * CH, CH), CH)
                d = [dt[tile[l], row, :] for l in range(lw)]
                du = [ut[tile[l], row, :] for l in range(lw)]
                out = []
                for n in range(NG):
                    w = wx[n, row, :]
                    for l in range(lw):
                        a = jnp.exp2(d[l] * rate[n][l])
                        ab[n * lw + l, row, :] = a
                        out.append(a * h[n * lw + l] + w * du[l])
                return tuple(out), tuple(cum[l] + d[l] for l in range(lw))

            h, cum = lax.fori_loop(
                0, chunk, first, ((zero,) * (NG * lw), (zero,) * lw), unroll=2
            )
            start = []
            for n in range(NG):
                for l in range(lw):
                    h0 = h0_ref[g * NG + n : g * NG + n + 1, lanes[l]]
                    p, hh = _link(jnp.exp2(cum[l] * rate[n][l]), h[n * lw + l], False)
                    full = hh + p * h0
                    begin = jnp.where(_rows_mask(1, False), pltpu.roll(full, 1, 0), h0)
                    hin_ref[g * NG + n, :, lanes[l]] = begin
                    hend_ref[g * NG + n : g * NG + n + 1, lanes[l]] = full[CH - 1 : CH]
                    start.append(begin)

            def second(t, h):
                row = pl.ds(pl.multiple_of(t * CH, CH), CH)
                du = [ut[tile[l], row, :] for l in range(lw)]
                out = []
                y = [None] * lw
                for n in range(NG):
                    w = wx[n, row, :]
                    r = rx[n, row, :]
                    for l in range(lw):
                        a = ab[n * lw + l, row, :]
                        hn = a * h[n * lw + l] + w * du[l]
                        out.append(hn)
                        y[l] = r * hn if n == 0 else y[l] + r * hn
                for l in range(lw):
                    yt[tile[l], row, :] = y[l] if g == 0 else yt[tile[l], row, :] + y[l]
                return tuple(out)

            lax.fori_loop(0, chunk, second, tuple(start), unroll=2)
    _unweave(y_ref, yt, chunk)


def scan_fwd(delta, inner, pick, a2, h0, rank, state):
    length, el = delta.shape
    chunk = length // CH
    lw = 2 if el % 256 == 0 else 1
    f32 = jnp.float32
    return pl.pallas_call(
        functools.partial(fwd_kernel, chunk, lw, rank, state),
        out_shape=(
            jax.ShapeDtypeStruct((length, el), f32),
            jax.ShapeDtypeStruct((state, CH, el), f32),
            jax.ShapeDtypeStruct((state, el), f32),
        ),
        in_specs=[pl.BlockSpec(memory_space=pltpu.VMEM)] * 5,
        out_specs=[pl.BlockSpec(memory_space=pltpu.VMEM)] * 3,
        scratch_shapes=[
            pltpu.VMEM((NG, length, 128), f32),
            pltpu.VMEM((NG, length, 128), f32),
            pltpu.VMEM((NG * lw, length, 128), f32),
        ]
        + [pltpu.VMEM((el // 128, length, 128), f32)] * 3,
        compiler_params=pltpu.CompilerParams(vmem_limit_bytes=60 << 20),
        name="scan_fwd",
    )(delta, inner, pick, a2, h0)


def bwd_kernel(chunk, lw, rank, state, delta_ref, inner_ref, gs_ref, pick_ref, a2_ref, hin_ref, k0_ref, s1_ref, s2_ref, gd_ref, gwr_ref, kend_ref, wx, rx, gw, gr, ab, hb, dt, ut, gt, s1t, s2t):
    el = delta_ref.shape[1]
    _weave(dt, lambda i, j: delta_ref[i, j], chunk)
    _weave(ut, lambda i, j: delta_ref[i, j] * inner_ref[i, j], chunk)
    _weave(gt, lambda i, j: gs_ref[i, j], chunk)
    for g in range(state // NG):
        _expand(wx, pick_ref, rank, g * NG, chunk)
        _expand(rx, pick_ref, rank + state, g * NG, chunk)
        for q in range(el // (128 * lw)):
            tile = [q * lw + l for l in range(lw)]
            lanes = [slice((q * lw + l) * 128, (q * lw + l + 1) * 128) for l in range(lw)]
            rate = [[a2_ref[g * NG + n : g * NG + n + 1, lanes[l]] for l in range(lw)] for n in range(NG)]
            zero = jnp.zeros((CH, 128), jnp.float32)
            begin = []
            for n in range(NG):
                for l in range(lw):
                    h = hin_ref[g * NG + n, :, lanes[l]]
                    hb[n * lw + l, 0:CH, :] = h
                    begin.append(h)

            def ahead(t, carry):
                h, cum = carry
                row = pl.ds(pl.multiple_of(t * CH, CH), CH)
                d = [dt[tile[l], row, :] for l in range(lw)]
                du = [ut[tile[l], row, :] for l in range(lw)]
                later = pl.ds(pl.multiple_of(t * CH + CH, CH), CH)
                out = []
                for n in range(NG):
                    w = wx[n, row, :]
                    for l in range(lw):
                        col = n * lw + l
                        a = jnp.exp2(d[l] * rate[n][l])
                        ab[col, row, :] = a
                        hn = a * h[n * lw + l] + w * du[l]
                        hb[col, later, :] = hn
                        out.append(hn)
                return tuple(out), tuple(cum[l] + d[l] for l in range(lw))

            unused, cum = lax.fori_loop(
                0, chunk, ahead, (tuple(begin), (zero,) * lw), unroll=2
            )

            def local(i, k):
                t = chunk - 1 - i
                row = pl.ds(pl.multiple_of(t * CH, CH), CH)
                gs = [gt[tile[l], row, :] for l in range(lw)]
                out = []
                for n in range(NG):
                    r = rx[n, row, :]
                    for l in range(lw):
                        col = n * lw + l
                        out.append(ab[col, row, :] * (k[n * lw + l] + r * gs[l]))
                return tuple(out)

            k = lax.fori_loop(0, chunk, local, (zero,) * (NG * lw), unroll=2)
            start = []
            for n in range(NG):
                for l in range(lw):
                    k0 = k0_ref[g * NG + n : g * NG + n + 1, lanes[l]]
                    p, kk = _link(jnp.exp2(cum[l] * rate[n][l]), k[n * lw + l], True)
                    full = kk + p * k0
                    start.append(jnp.where(_rows_mask(1, True), pltpu.roll(full, CH - 1, 0), k0))
                    kend_ref[g * NG + n : g * NG + n + 1, lanes[l]] = full[0:1]

            def final(i, carry):
                k, gd = carry
                t = chunk - 1 - i
                row = pl.ds(pl.multiple_of(t * CH, CH), CH)
                d = [dt[tile[l], row, :] for l in range(lw)]
                du = [ut[tile[l], row, :] for l in range(lw)]
                gs = [gt[tile[l], row, :] for l in range(lw)]
                later = pl.ds(pl.multiple_of(t * CH + CH, CH), CH)
                ko, gdo = [], []
                s1 = [None] * lw
                s2 = [None] * lw
                for n in range(NG):
                    w = wx[n, row, :]
                    r = rx[n, row, :]
                    gwn = grn = None
                    for l in range(lw):
                        col = n * lw + l
                        gh = k[n * lw + l] + r * gs[l]
                        kn = ab[col, row, :] * gh
                        q_ = kn * hb[col, row, :]
                        ko.append(kn)
                        gdo.append(gd[n * lw + l] + q_ * d[l])
                        f1 = rate[n][l] * q_
                        f2 = gh * w
                        s1[l] = f1 if n == 0 else s1[l] + f1
                        s2[l] = f2 if n == 0 else s2[l] + f2
                        gwn = gh * du[l] if l == 0 else gwn + gh * du[l]
                        hr = gs[l] * hb[col, later, :]
                        grn = hr if l == 0 else grn + hr
                    gw[n, row, :] = gwn if q == 0 else gw[n, row, :] + gwn
                    gr[n, row, :] = grn if q == 0 else gr[n, row, :] + grn
                for l in range(lw):
                    s1t[tile[l], row, :] = s1[l] if g == 0 else s1t[tile[l], row, :] + s1[l]
                    s2t[tile[l], row, :] = s2[l] if g == 0 else s2t[tile[l], row, :] + s2[l]
                return tuple(ko), tuple(gdo)

            unused, gd = lax.fori_loop(
                0, chunk, final, (tuple(start), (zero,) * (NG * lw)), unroll=1
            )
            for n in range(NG):
                for l in range(lw):
                    gd_ref[g * NG + n : g * NG + n + 1, lanes[l]] = jnp.sum(gd[n * lw + l], axis=0, keepdims=True)

        c_at = lax.broadcasted_iota(jnp.int32, (2 * state, 128), 0)
        for c in range(CH):
            rows = pl.ds(c, chunk, stride=CH)
            here = slice(c * chunk, (c + 1) * chunk)
            part = None if g == 0 else gwr_ref[:, here]
            for n in range(NG):
                for src, base in ((gw, 0), (gr, state)):
                    ones = jnp.where(c_at == base + g * NG + n, 1.0, 0.0).astype(jnp.bfloat16)
                    one = lax.dot_general(
                        ones,
                        src.at[n][rows, :].astype(jnp.bfloat16),
                        (((1,), (1,)), ((), ())),
                        preferred_element_type=jnp.float32,
                    )
                    part = one if part is None else part + one
            gwr_ref[:, here] = part
    _unweave(s1_ref, s1t, chunk)
    _unweave(s2_ref, s2t, chunk)


def scan_bwd(delta, inner, gs, pick, a2, hin, k0, rank, state):
    length, el = delta.shape
    chunk = length // CH
    lw = 2 if el % 256 == 0 else 1
    f32 = jnp.float32
    return pl.pallas_call(
        functools.partial(bwd_kernel, chunk, lw, rank, state),
        out_shape=(
            jax.ShapeDtypeStruct((length, el), f32),
            jax.ShapeDtypeStruct((length, el), f32),
            jax.ShapeDtypeStruct((state, el), f32),
            jax.ShapeDtypeStruct((2 * state, length), f32),
            jax.ShapeDtypeStruct((state, el), f32),
        ),
        in_specs=[pl.BlockSpec(memory_space=pltpu.VMEM)] * 7,
        out_specs=[pl.BlockSpec(memory_space=pltpu.VMEM)] * 5,
        scratch_shapes=[pltpu.VMEM((NG, length, 128), f32)] * 4
        + [
            pltpu.VMEM((NG * lw, length, 128), f32),
            pltpu.VMEM((NG * lw, length + CH, 128), f32),
        ]
        + [pltpu.VMEM((el // 128, length, 128), f32)] * 5,
        compiler_params=pltpu.CompilerParams(vmem_limit_bytes=63 << 20),
        name="scan_bwd",
    )(delta, inner, gs, pick, a2, hin, k0)


EPS = 1e-05
LN2 = 0.6931471805599453
SEGMENT = 1024
BF = jnp.bfloat16
F32 = jnp.float32


def peers_barrier(seq_peers, dp_peers):
    barrier = pltpu.get_barrier_semaphore()
    for p in seq_peers:
        pl.semaphore_signal(barrier, inc=1, device_id={"seq": p}, device_id_type=MESH)
    for p in dp_peers:
        pl.semaphore_signal(barrier, inc=1, device_id={"dp": p}, device_id_type=MESH)
    pl.semaphore_wait(barrier, len(seq_peers) + len(dp_peers))


def sum_kernel(n, part_ref, out_ref, recv, send_sem, recv_sem, back_send, back_recv):
    me = lax.axis_index("seq")
    peers = [lax.rem(me + k, n) for k in range(1, n)]
    peers_barrier(peers, [])

    def at(p):
        return pl.ds(pl.multiple_of(p * 128, 128), 128)

    out = [
        pltpu.make_async_remote_copy(
            src_ref=part_ref.at[:, at(p)],
            dst_ref=recv.at[k],
            send_sem=send_sem.at[k],
            recv_sem=recv_sem.at[k],
            device_id={"seq": p},
            device_id_type=MESH,
        )
        for k, p in enumerate(peers)
    ]
    for c in out:
        c.start()
    total = part_ref[:, at(me)].astype(F32)
    for k, c in enumerate(out):
        c.wait_recv()
        total = total + recv[k].astype(F32)
    out_ref[:, at(me)] = total.astype(BF)
    back = [
        pltpu.make_async_remote_copy(
            src_ref=out_ref.at[:, at(me)],
            dst_ref=out_ref.at[:, at(me)],
            send_sem=back_send.at[k],
            recv_sem=back_recv.at[k],
            device_id={"seq": p},
            device_id_type=MESH,
        )
        for k, p in enumerate(peers)
    ]
    for c in back:
        c.start()
    for c in out:
        c.wait_send()
    for c in back:
        c.wait()


def sum_over_seq(part, n, name, ident):
    rows, length = part.shape
    return pl.pallas_call(
        functools.partial(sum_kernel, n),
        out_shape=jax.ShapeDtypeStruct((rows, length), BF),
        in_specs=[pl.BlockSpec(memory_space=pltpu.VMEM)],
        out_specs=pl.BlockSpec(memory_space=pltpu.VMEM),
        scratch_shapes=[pltpu.VMEM((n - 1, rows, 128), BF)] + [pltpu.SemaphoreType.DMA((n - 1,))] * 4,
        compiler_params=pltpu.CompilerParams(collective_id=ident, has_side_effects=True),
        name=name,
    )(part)


SLAB = 32


def front_kernel(xn, wp, pk, xg, wg, pg, local_sem, z_send, z_recv, y_send, y_recv, w_send, w_recv, d_send, d_recv, p_send, p_recv):
    s = lax.axis_index("seq")
    d = lax.axis_index("dp")
    n = 8
    z, y = s // 2, lax.rem(s, 2)
    other = s + 1 - 2 * y
    cross = lax.rem(d + 2, 4)
    core = d + 1 - 2 * lax.rem(d, 2)
    peers = [lax.rem(s + k, n) for k in range(1, n)]
    peers_barrier(peers, [cross, core])
    col = xn.shape[0] // SLAB

    def slab(c):
        return pl.ds(c * SLAB, SLAB)

    own = [
        pltpu.make_async_copy(xn, xg.at[s], local_sem.at[0]),
        pltpu.make_async_copy(wp.at[s], wg.at[d, s], local_sem.at[1]),
        pltpu.make_async_copy(pk, pg.at[d], local_sem.at[2]),
    ]

    def copy(src, dst, ss, rs, to):
        return pltpu.make_async_remote_copy(
            src_ref=src, dst_ref=dst, send_sem=ss, recv_sem=rs, device_id=to, device_id_type=MESH
        )

    chains = [(c, y) for c in range(col)] + [(col - 1, 1 - y)]

    def z_copy(chain, up, j):
        c, yy = chains[chain]
        block = (z - j if up else z + j) * 2 + yy
        src = xn.at[slab(c)] if (j == 0 and chain < col) else xg.at[block, slab(c)]
        at = chain * 6 + (0 if up else 3) + j
        return copy(src, xg.at[block, slab(c)], z_send.at[at], z_recv.at[at], {"seq": s + 2 if up else s - 2})

    def z_arrived(chain, up, j):
        c, yy = chains[chain]
        block = (z - j if up else z + j) * 2 + yy
        at = chain * 6 + (0 if up else 3) + j - 1
        ref = xg.at[block, slab(c)]
        return copy(ref, ref, z_send.at[at], z_recv.at[at], {"seq": s})

    def can(up, j):
        return z >= j if up else z <= 3 - j

    def can_send(up):
        return z < 3 if up else z > 0

    def y_copy(chain, where):
        c = chains[chain][0]
        block = (z + where) * 2 + y
        src = xn.at[slab(c)] if where == 0 else xg.at[block, slab(c)]
        at = chain * 7 + where + 3
        return copy(src, xg.at[block, slab(c)], y_send.at[at], y_recv.at[at], {"seq": other})

    def w_copy(k):
        return copy(wp.at[peers[k]], wg.at[d, s], w_send.at[k], w_recv.at[k], {"seq": peers[k]})

    def w_from(k):
        source = lax.rem(s + n - 1 - k, n)
        ref = wg.at[d, source]
        return copy(ref, ref, w_send.at[k], w_recv.at[k], {"seq": s}), source

    def d_copy(k, source, kind):
        block = cross if kind == 2 else d
        src = wp.at[s] if (k == 7 and kind < 2) else wg.at[block, source]
        at = k * 3 + kind
        return copy(src, wg.at[block, source], d_send.at[at], d_recv.at[at], {"dp": cross if kind == 0 else core})

    def d_from(k, source, kind):
        block = cross if kind == 0 else (core if kind == 1 else 3 - d)
        return block

    def p_copy(c, kind):
        block = cross if kind == 2 else d
        rows = slab(c)
        src = pk.at[rows] if kind < 2 else pg.at[block, rows]
        at = c * 3 + kind
        return copy(src, pg.at[block, rows], p_send.at[at], p_recv.at[at], {"dp": cross if kind == 0 else core})

    for k in range(n - 1):
        w_copy(k).start()
    y_copy(col - 1, 0).start()
    for chain in range(col):
        for up in (True, False):

            @pl.when(can_send(up))
            def _():
                z_copy(chain, up, 0).start()

        if chain < col - 1:
            y_copy(chain, 0).start()
    for kind in (0, 1):
        d_copy(7, s, kind).start()
    for c in range(col):
        for kind in (0, 1):
            p_copy(c, kind).start()
    for c in own:
        c.start()

    sources = []
    for k in range(n - 1):
        sources.append(lax.rem(s + n - 1 - k, n))
    sources.append(s)

    def w_relay(k):
        arrived, source = w_from(k)
        arrived.wait_recv()
        for kind in (0, 1):
            d_copy(k, source, kind).start()

    def cross_relay(k):
        source = sources[k]
        ref = wg.at[cross, source]
        copy(ref, ref, d_send.at[k * 3], d_recv.at[k * 3], {"seq": s}).wait_recv()
        d_copy(k, source, 2).start()

    def z_round(j):
        for chain in range(col + 1):
            for up in (True, False):

                @pl.when(can(up, j))
                def _():
                    z_arrived(chain, up, j).wait_recv()
                    if j < 3:

                        @pl.when(can_send(up))
                        def _():
                            z_copy(chain, up, j).start()

                    if chain < col - 1:
                        y_copy(chain, -j if up else j).start()

    def y_arrived(chain, where):
        c = chains[chain][0]
        ref = xg.at[(z + where) * 2 + 1 - y, slab(c)]
        at = chain * 7 + where + 3
        return copy(ref, ref, y_send.at[at], y_recv.at[at], {"seq": s})

    y_arrived(col - 1, 0).wait_recv()
    for up in (True, False):

        @pl.when(can_send(up))
        def _():
            z_copy(col, up, 0).start()

    z_round(1)
    for k in (0, 1, 5, 6):
        w_relay(k)
    z_round(2)
    for k in (2, 3, 4):
        w_relay(k)
    for c in range(col):
        ref = pg.at[cross, slab(c)]
        copy(ref, ref, p_send.at[c * 3], p_recv.at[c * 3], {"seq": s}).wait_recv()
        p_copy(c, 2).start()
    z_round(3)
    for k in (7, 0, 1, 5, 6, 2, 3, 4):
        cross_relay(k)
    for chain in range(col - 1):
        y_arrived(chain, 0).wait_recv()
        for j in (1, 2, 3):
            for up in (True, False):

                @pl.when(can(up, j))
                def _():
                    y_arrived(chain, -j if up else j).wait_recv()

    diag = lax.rem(core + 2, 4)
    for k in range(n):
        for kind, block in ((1, core), (2, diag)):
            ref = wg.at[block, sources[k]]
            at = k * 3 + kind
            copy(ref, ref, d_send.at[at], d_recv.at[at], {"seq": s}).wait_recv()
    for c in range(col):
        for kind, block in ((1, core), (2, diag)):
            ref = pg.at[block, slab(c)]
            at = c * 3 + kind
            copy(ref, ref, p_send.at[at], p_recv.at[at], {"seq": s}).wait_recv()
    for k in range(n - 1):
        w_copy(k).wait_send()
    for k in range(n):
        for kind in (0, 1, 2):
            d_copy(k, sources[k], kind).wait_send()
    for c in range(col):
        for kind in (0, 1, 2):
            p_copy(c, kind).wait_send()
    y_copy(col - 1, 0).wait_send()
    for chain in range(col - 1):
        y_copy(chain, 0).wait_send()
        for j in (1, 2, 3):
            for up in (True, False):

                @pl.when(can(up, j))
                def _():
                    y_copy(chain, -j if up else j).wait_send()

    for chain in range(col + 1):
        for up in (True, False):

            @pl.when(can_send(up))
            def _():
                z_copy(chain, up, 0).wait_send()

            for j in (1, 2):

                @pl.when(jnp.logical_and(can(up, j), can_send(up)))
                def _():
                    z_copy(chain, up, j).wait_send()

    for c in own:
        c.wait()


def front_gather(xn, wp, pk):
    col = xn.shape[0] // SLAB
    dma = pltpu.SemaphoreType.DMA
    return pl.pallas_call(
        front_kernel,
        out_shape=(
            jax.ShapeDtypeStruct((8,) + xn.shape, BF),
            jax.ShapeDtypeStruct((4,) + wp.shape, BF),
            jax.ShapeDtypeStruct((4,) + pk.shape, BF),
        ),
        in_specs=[pl.BlockSpec(memory_space=pltpu.VMEM)] * 3,
        out_specs=[pl.BlockSpec(memory_space=pltpu.VMEM)] * 3,
        scratch_shapes=[
            dma((3,)),
            dma(((col + 1) * 6,)),
            dma(((col + 1) * 6,)),
            dma((col * 7,)),
            dma((col * 7,)),
            dma((7,)),
            dma((7,)),
            dma((24,)),
            dma((24,)),
            dma((col * 3,)),
            dma((col * 3,)),
        ],
        compiler_params=pltpu.CompilerParams(
            collective_id=3, has_side_effects=True, vmem_limit_bytes=40 << 20
        ),
        name="front_gather",
    )(xn, wp, pk)


def silu_slope(values_in):
    sigmoid_value = jax.nn.sigmoid(values_in)
    return sigmoid_value * (1.0 + values_in * (1.0 - sigmoid_value))


def dot(a, b, dims):
    return lax.dot_general(a, b, (dims, ((), ())), preferred_element_type=F32)


def segments(length):
    count = max(1, length // SEGMENT)
    size = length // count
    return [(i * size, (i + 1) * size) for i in range(count)]


def forward_scan(step_size, inner, picked, rate2):
    state = rate2.shape[0]
    carry = jnp.zeros(rate2.shape, F32)
    outs, starts = [], []
    for lo, hi in segments(step_size.shape[0]):
        y, start, carry = scan_fwd(step_size[lo:hi], inner[lo:hi], picked[:, lo:hi], rate2, carry, RANK, state)
        outs.append(y)
        starts.append(start)
    return (outs[0] if len(outs) == 1 else jnp.concatenate(outs, axis=0)), starts


def backward_scan(step_size, inner, grad_scan, picked, rate2, starts):
    state = rate2.shape[0]
    carry = jnp.zeros(rate2.shape, F32)
    parts = []
    total = jnp.zeros(rate2.shape, F32)
    spans = segments(step_size.shape[0])
    for (lo, hi), start in reversed(list(zip(spans, starts))):
        s1, s2, decay, gwr, carry = scan_bwd(
            step_size[lo:hi], inner[lo:hi], grad_scan[lo:hi], picked[:, lo:hi], rate2, start, carry, RANK, state
        )
        total = total + decay
        parts.append((s1, s2, gwr))
    parts = parts[::-1]
    if len(parts) == 1:
        s1, s2, gwr = parts[0]
    else:
        s1, s2, gwr = (jnp.concatenate(p, axis=k) for k, p in zip((0, 0, 1), zip(*parts)))
    return s1, s2, gwr, total


def shards(
    block_input,
    norm_gain,
    in_weight,
    conv_weight,
    conv_bias,
    select_weight,
    step_weight,
    step_bias,
    decay_log,
    skip_gain,
    out_weight,
    output_grad,
):
    n_dp, n_seq = lax.axis_size("dp"), lax.axis_size("seq")
    token_rows = block_input[0]
    upstream_rows = output_grad[0]
    width = token_rows.shape[1]
    d_rows = in_weight.shape[0]
    e_rows = out_weight.shape[0]
    local = n_dp * e_rows

    own = token_rows.astype(F32)
    own_scale = lax.rsqrt(jnp.mean(own * own, axis=1, keepdims=True) + EPS)
    own_normed = (own * own_scale).astype(BF)
    gain = norm_gain.astype(F32)[:, None]
    pieces = (in_weight.astype(F32) * gain).astype(BF)
    pieces = pieces.reshape(d_rows, 2, n_dp, n_seq, e_rows).transpose(3, 0, 1, 2, 4).reshape(n_seq, d_rows, 2 * local)

    smalls = [select_weight, step_weight, decay_log, conv_weight, conv_bias[:, None], step_bias[:, None], skip_gain[:, None]]
    used = sum(s.shape[1] for s in smalls)
    pad = -used % 128
    packed = jnp.concatenate([out_weight] + smalls + [jnp.zeros((e_rows, pad), BF)], axis=1)
    if (n_dp, n_seq) == (4, 8):
        normed, in_w, packed = front_gather(own_normed, pieces, packed)
        packed = packed.reshape(local, packed.shape[2])
    else:
        normed = lax.all_gather(own_normed, "seq")
        in_w = lax.all_gather(lax.all_to_all(pieces, "seq", 0, 0), "dp")
        packed = lax.all_gather(packed, "dp", axis=0, tiled=True)
    length = n_seq * token_rows.shape[0]
    normed = normed.reshape(length, width)
    in_w = in_w.reshape(width, 2 * local)
    upstream_rows, normed = lax.optimization_barrier((upstream_rows, normed))
    cuts = []
    begin = 0
    for s in [out_weight] + smalls:
        cuts.append((begin, begin + s.shape[1]))
        begin += s.shape[1]
    out_w, sel_w, step_w, dec_w, conv_w, conv_b, step_b, skip = (packed[:, a:b] for a, b in cuts)
    conv_taps = conv_w.astype(F32).T
    conv_b, step_b, skip = (v[:, 0].astype(F32) for v in (conv_b, step_b, skip))
    decay_rate = -jnp.exp(dec_w.astype(F32).T)
    rate2 = decay_rate * (1.0 / LN2)

    mixed = dot(normed, in_w, ((1,), (0,))).astype(BF)
    padded = jnp.concatenate([jnp.zeros((KERNEL - 1, local), BF), mixed[:, :local]], axis=0).astype(F32)
    gate_in = mixed[:, local:].astype(F32)
    conv_out = conv_b + jnp.zeros((length, local), F32)
    for offset in range(KERNEL):
        conv_out = conv_out + padded[offset : offset + length] * conv_taps[offset]
    inner = jax.nn.silu(conv_out).astype(BF)
    inner_f = inner.astype(F32)
    picked = sum_over_seq(dot(sel_w, inner, ((0,), (1,))).astype(BF), n_seq, "sum_picked", 1)
    step_in = picked[:RANK]
    step_raw = dot(step_in, step_w, ((0,), (1,))) + step_b
    step_size = jax.nn.softplus(step_raw)
    scanned, starts = forward_scan(step_size, inner_f, picked, rate2)
    mamba_out = scanned + skip * inner_f
    gate_act = jax.nn.silu(gate_in)
    gated_out = (mamba_out * gate_act).astype(BF)
    out_part = dot(gated_out, out_w, ((1,), (0,))).astype(BF)

    upstream = lax.all_gather(upstream_rows, "seq", axis=0, tiled=True)
    grad_gated = dot(upstream, out_w, ((1,), (1,)))
    grad_out_w = dot(gated_out, upstream, ((0,), (0,)))
    grad_scan = grad_gated * gate_act
    grad_gate = grad_gated * mamba_out * silu_slope(gate_in)
    grad_skip = jnp.sum(grad_scan * inner_f, axis=0)
    grad_scan, out_part = lax.optimization_barrier((grad_scan, out_part))
    s1, s2, grad_wr, grad_decay = backward_scan(step_size, inner_f, grad_scan, picked, rate2, starts)
    out_rows = lax.psum_scatter(out_part, "seq", scatter_dimension=0, tiled=True)
    layer_out = (token_rows.astype(F32) + out_rows.astype(F32)).astype(BF)
    grad_raw_f = (s1 * LN2 + inner_f * s2) * jax.nn.sigmoid(step_raw)
    grad_step_b = jnp.sum(grad_raw_f, axis=0)
    grad_raw = grad_raw_f.astype(BF)
    grad_step_w = dot(grad_raw, step_in, ((0,), (1,)))
    part = jnp.concatenate([dot(step_w, grad_raw, ((0,), (1,))), grad_wr], axis=0).astype(BF)
    grad_picked = sum_over_seq(part, n_seq, "sum_grad_picked", 2)
    grad_sel = dot(inner, grad_picked, ((0,), (1,)))
    grad_inner = step_size * s2 + grad_scan * skip + dot(grad_picked, sel_w, ((0,), (1,)))
    grad_conv = grad_inner * silu_slope(conv_out)
    grad_conv_b = jnp.sum(grad_conv, axis=0)
    grad_taps = [jnp.sum(grad_conv * padded[k : k + length], axis=0) for k in range(KERNEL)]
    extended = jnp.concatenate([grad_conv, jnp.zeros((KERNEL - 1, local), F32)], axis=0)
    grad_conv_in = jnp.zeros((length, local), F32)
    for k in range(KERNEL):
        grad_conv_in = grad_conv_in + extended[KERNEL - 1 - k : KERNEL - 1 - k + length] * conv_taps[k]
    grad_mixed = jnp.concatenate([grad_conv_in, grad_gate], axis=1).astype(BF)
    grad_in_w = dot(normed, grad_mixed, ((0,), (0,)))
    grad_normed = dot(grad_mixed, in_w, ((1,), (1,)))

    small_grads = [grad_sel, grad_step_w, (grad_decay * decay_rate).T, jnp.stack(grad_taps, axis=1), grad_conv_b[:, None], grad_step_b[:, None], grad_skip[:, None]]
    packed_grad = jnp.concatenate([grad_out_w] + small_grads + [jnp.zeros((local, pad), F32)], axis=1).astype(BF)
    packed_grad = lax.psum_scatter(packed_grad, "dp", scatter_dimension=0, tiled=True).astype(F32)
    g_out, g_sel, g_step, g_dec, g_conv, g_cb, g_sb, g_skip = (packed_grad[:, a:b] for a, b in cuts)

    grad_in_all = lax.psum_scatter(grad_in_w.astype(BF), "dp", scatter_dimension=0, tiled=True)
    grad_in_all = lax.all_to_all(grad_in_all, "seq", split_axis=0, concat_axis=0, tiled=True)
    grad_in_all = grad_in_all.reshape(n_seq, d_rows, 2, n_dp, e_rows).transpose(1, 2, 3, 0, 4).reshape(in_weight.shape).astype(F32)
    g_gain = jnp.sum(grad_in_all * in_weight.astype(F32), axis=1)
    g_in = grad_in_all * gain

    grad_normed = lax.psum_scatter(grad_normed.astype(BF), "seq", scatter_dimension=0, tiled=True).astype(F32)
    scaled = grad_normed
    grad_rows = own_scale * scaled - own * (own_scale * own_scale * own_scale) * jnp.mean(scaled * own, axis=1, keepdims=True)
    input_grad = (upstream_rows.astype(F32) + grad_rows).astype(BF)
    return (
        layer_out[None],
        input_grad[None],
        g_gain,
        g_in,
        g_conv,
        g_cb[:, 0],
        g_sel,
        g_step,
        g_sb[:, 0],
        g_dec,
        g_skip[:, 0],
        g_out,
    )


def solution(mesh):
    rows = P(("dp", "seq"))
    both = P(("dp", "seq"), None)
    acts = P("dp", "seq", None)
    return jax.shard_map(
        shards,
        mesh=mesh,
        in_specs=(acts, rows, both, both, rows, both, both, rows, both, rows, both, acts),
        out_specs=(acts, acts, rows, both, both, rows, both, both, rows, both, rows, both),
        check_vma=False,
    )
```

```python
import functools
import jax
import jax.numpy as jnp
from jax import lax
from jax.experimental import pallas as pl
from jax.experimental.pallas import tpu as pltpu
from jax.sharding import PartitionSpec as P

RANK = 128
KERNEL = 4
MESH = pl.DeviceIdType.MESH
HIDE = True
BF = jnp.bfloat16
F32 = jnp.float32

CH = 8


def _expand(dst, pick_ref, base, first, chunk):
    ng = dst.shape[0]
    cols = pick_ref.shape[0]
    width = ng * 128
    k_at = lax.broadcasted_iota(jnp.int32, (cols, width), 0)
    n_at = lax.broadcasted_iota(jnp.int32, (cols, width), 1) // 128
    pick_one = jnp.where(k_at == base + first + n_at, 1.0, 0.0).astype(BF)
    for c in range(CH):
        tokens = pick_ref[:, c * chunk : (c + 1) * chunk]
        wide = lax.dot_general(
            tokens, pick_one, (((0,), (0,)), ((), ())), preferred_element_type=F32
        )
        for n in range(ng):
            dst.at[n][pl.ds(c, chunk, stride=CH), :] = wide[:, n * 128 : (n + 1) * 128]


def _weave(dst, value, chunk):
    for q in range(dst.shape[0]):
        for c in range(CH):
            dst.at[q][pl.ds(c, chunk, stride=CH), :] = value(
                slice(c * chunk, (c + 1) * chunk), slice(q * 128, (q + 1) * 128)
            )


def _unweave(dst, src, chunk):
    for q in range(src.shape[0]):
        for c in range(CH):
            dst[c * chunk : (c + 1) * chunk, q * 128 : (q + 1) * 128] = src.at[q][
                pl.ds(c, chunk, stride=CH), :
            ]


def _rows_mask(k, up):
    row = lax.broadcasted_iota(jnp.int32, (CH, 128), 0)
    return row < CH - k if up else row >= k


def _link(p, h, up):
    for k in (1, 2, 4):
        mask = _rows_mask(k, up)
        shift = CH - k if up else k
        ps = jnp.where(mask, pltpu.roll(p, shift, 0), 1.0)
        hs = jnp.where(mask, pltpu.roll(h, shift, 0), 0.0)
        h = h + p * hs
        p = p * ps
    return p, h


def _split_loop(total, parts, body, carry, unroll, point):
    size = total // parts
    for i in range(parts):
        carry = lax.fori_loop(i * size, (i + 1) * size, body, carry, unroll=unroll)
        point()
    return carry


def fwd_kernel(chunk, lw, ng, rank, state, hide, *refs):
    delta_ref, inner_ref, pick_ref, a2_ref, h0_ref = refs[:5]
    refs = refs[5:]
    extra_in, refs = refs[:hide], refs[hide:]
    y_ref, hin_ref, hend_ref = refs[:3]
    refs = refs[3:]
    extra_out, refs = refs[:hide], refs[hide:]
    wx, rx, ab, dt, ut, yt = refs[:6]
    todo = []
    if hide:
        sems = refs[6:10]
        local_sem = refs[10]
        s = lax.axis_index("seq")
        d = lax.axis_index("dp")
        peers_barrier([lax.rem(s + k, 8) for k in range(1, 8)], [lax.rem(d + 2, 4), d + 1 - 2 * lax.rem(d, 2)])
        start, steps, finish = gather_stages(extra_in[0], extra_out[0], *sems)
        start()
        own = pltpu.make_async_copy(extra_in[0], extra_out[0].at[s], local_sem)
        own.start()
        skip = lambda: None
        todo = [steps[0], skip, steps[1], skip, steps[2], skip, steps[3], skip]

    def point():
        if todo:
            todo.pop(0)()

    el = delta_ref.shape[1]
    _weave(dt, lambda i, j: delta_ref[i, j], chunk)
    _weave(ut, lambda i, j: delta_ref[i, j] * inner_ref[i, j], chunk)
    for g in range(state // ng):
        _expand(wx, pick_ref, rank, g * ng, chunk)
        _expand(rx, pick_ref, rank + state, g * ng, chunk)
        for q in range(el // (128 * lw)):
            tile = [q * lw + l for l in range(lw)]
            lanes = [slice((q * lw + l) * 128, (q * lw + l + 1) * 128) for l in range(lw)]
            rate = [[a2_ref[g * ng + n : g * ng + n + 1, lanes[l]] for l in range(lw)] for n in range(ng)]
            zero = jnp.zeros((CH, 128), F32)

            def first(t, carry):
                h, cum = carry
                row = pl.ds(pl.multiple_of(t * CH, CH), CH)
                d = [dt[tile[l], row, :] for l in range(lw)]
                du = [ut[tile[l], row, :] for l in range(lw)]
                out = []
                for n in range(ng):
                    w = wx[n, row, :]
                    for l in range(lw):
                        a = jnp.exp2(d[l] * rate[n][l])
                        ab[n * lw + l, row, :] = a
                        out.append(a * h[n * lw + l] + w * du[l])
                return tuple(out), tuple(cum[l] + d[l] for l in range(lw))

            h, cum = _split_loop(chunk, 1, first, ((zero,) * (ng * lw), (zero,) * lw), 4, point)
            begin_at = []
            for n in range(ng):
                for l in range(lw):
                    h0 = h0_ref[g * ng + n : g * ng + n + 1, lanes[l]]
                    p, hh = _link(jnp.exp2(cum[l] * rate[n][l]), h[n * lw + l], False)
                    full = hh + p * h0
                    begin = jnp.where(_rows_mask(1, False), pltpu.roll(full, 1, 0), h0)
                    hin_ref[g * ng + n, :, lanes[l]] = begin
                    hend_ref[g * ng + n : g * ng + n + 1, lanes[l]] = full[CH - 1 : CH]
                    begin_at.append(begin)

            def second(t, h):
                row = pl.ds(pl.multiple_of(t * CH, CH), CH)
                du = [ut[tile[l], row, :] for l in range(lw)]
                out = []
                y = [None] * lw
                for n in range(ng):
                    w = wx[n, row, :]
                    r = rx[n, row, :]
                    for l in range(lw):
                        a = ab[n * lw + l, row, :]
                        hn = a * h[n * lw + l] + w * du[l]
                        out.append(hn)
                        y[l] = r * hn if n == 0 else y[l] + r * hn
                for l in range(lw):
                    yt[tile[l], row, :] = y[l] if g == 0 else yt[tile[l], row, :] + y[l]
                return tuple(out)

            _split_loop(chunk, 1, second, tuple(begin_at), 4, point)
    while todo:
        point()
    _unweave(y_ref, yt, chunk)
    if hide:
        finish()
        own.wait()


def scan_fwd(delta, inner, pick, a2, h0, rank, state, shard=None):
    length, el = delta.shape
    chunk = length // CH
    lw = min(4, el // 128)
    ng = 4 if lw == 4 else 8
    f32 = F32
    vmem = pl.BlockSpec(memory_space=pltpu.VMEM)
    out_shape = [
        jax.ShapeDtypeStruct((length, el), f32),
        jax.ShapeDtypeStruct((state, CH, el), f32),
        jax.ShapeDtypeStruct((state, el), f32),
    ]
    out_specs = [vmem] * 3
    scratch = [
        pltpu.VMEM((ng, length, 128), f32),
        pltpu.VMEM((ng, length, 128), f32),
        pltpu.VMEM((ng * lw, length, 128), f32),
    ] + [pltpu.VMEM((el // 128, length, 128), f32)] * 3
    args = [delta, inner, pick, a2, h0]
    params = dict(vmem_limit_bytes=60 << 20)
    if shard is not None:
        args.append(shard)
        out_shape.append(jax.ShapeDtypeStruct((8,) + shard.shape, BF))
        out_specs.append(pl.BlockSpec(memory_space=pl.ANY))
        scratch += gather_sems(shard.shape[0]) + [pltpu.SemaphoreType.DMA]
        params.update(collective_id=5, has_side_effects=True)
    return pl.pallas_call(
        functools.partial(fwd_kernel, chunk, lw, ng, rank, state, 0 if shard is None else 1),
        out_shape=tuple(out_shape),
        in_specs=[vmem] * len(args),
        out_specs=tuple(out_specs),
        scratch_shapes=scratch,
        compiler_params=pltpu.CompilerParams(**params),
        name="scan_fwd",
    )(*args)


def bwd_kernel(chunk, lw, ng, rank, state, hide, *refs):
    delta_ref, inner_ref, gs_ref, pick_ref, a2_ref, hin_ref, k0_ref = refs[:7]
    refs = refs[7:]
    extra_in, refs = refs[:hide], refs[hide:]
    s1_ref, s2_ref, gd_ref, gwr_ref, kend_ref = refs[:5]
    refs = refs[5:]
    extra_out, refs = refs[:hide], refs[hide:]
    wx, rx, gw, gr, ab, hb, dt, ut, gt, s1t, s2t = refs[:11]
    todo = []
    if hide:
        s = lax.axis_index("seq")
        d = lax.axis_index("dp")
        peers_barrier([lax.rem(s + k, 8) for k in range(1, 8)], [lax.rem(d + 2, 4), d + 1 - 2 * lax.rem(d, 2)])
        start, todo, finish = scatter_stages(extra_in[0], extra_out[0], *refs[11:21])
        todo = list(todo)
        start()

    def point():
        if todo:
            todo.pop(0)()

    el = delta_ref.shape[1]
    _weave(dt, lambda i, j: delta_ref[i, j], chunk)
    _weave(ut, lambda i, j: delta_ref[i, j] * inner_ref[i, j], chunk)
    _weave(gt, lambda i, j: gs_ref[i, j], chunk)
    for g in range(state // ng):
        _expand(wx, pick_ref, rank, g * ng, chunk)
        _expand(rx, pick_ref, rank + state, g * ng, chunk)
        for q in range(el // (128 * lw)):
            tile = [q * lw + l for l in range(lw)]
            lanes = [slice((q * lw + l) * 128, (q * lw + l + 1) * 128) for l in range(lw)]
            rate = [[a2_ref[g * ng + n : g * ng + n + 1, lanes[l]] for l in range(lw)] for n in range(ng)]
            zero = jnp.zeros((CH, 128), F32)
            begin = []
            for n in range(ng):
                for l in range(lw):
                    h = hin_ref[g * ng + n, :, lanes[l]]
                    hb[n * lw + l, 0:CH, :] = h
                    begin.append(h)

            def ahead(t, carry):
                h, cum = carry
                row = pl.ds(pl.multiple_of(t * CH, CH), CH)
                d = [dt[tile[l], row, :] for l in range(lw)]
                du = [ut[tile[l], row, :] for l in range(lw)]
                later = pl.ds(pl.multiple_of(t * CH + CH, CH), CH)
                out = []
                for n in range(ng):
                    w = wx[n, row, :]
                    for l in range(lw):
                        col = n * lw + l
                        a = jnp.exp2(d[l] * rate[n][l])
                        ab[col, row, :] = a
                        hn = a * h[n * lw + l] + w * du[l]
                        hb[col, later, :] = hn
                        out.append(hn)
                return tuple(out), tuple(cum[l] + d[l] for l in range(lw))

            unused, cum = _split_loop(chunk, 1, ahead, (tuple(begin), (zero,) * lw), 4, point)

            def local(i, k):
                t = chunk - 1 - i
                row = pl.ds(pl.multiple_of(t * CH, CH), CH)
                gs = [gt[tile[l], row, :] for l in range(lw)]
                out = []
                for n in range(ng):
                    r = rx[n, row, :]
                    for l in range(lw):
                        col = n * lw + l
                        out.append(ab[col, row, :] * (k[n * lw + l] + r * gs[l]))
                return tuple(out)

            k = _split_loop(chunk, 1, local, (zero,) * (ng * lw), 4, point)
            begin_at = []
            for n in range(ng):
                for l in range(lw):
                    k0 = k0_ref[g * ng + n : g * ng + n + 1, lanes[l]]
                    p, kk = _link(jnp.exp2(cum[l] * rate[n][l]), k[n * lw + l], True)
                    full = kk + p * k0
                    begin_at.append(jnp.where(_rows_mask(1, True), pltpu.roll(full, CH - 1, 0), k0))
                    kend_ref[g * ng + n : g * ng + n + 1, lanes[l]] = full[0:1]

            def final(i, carry):
                k, gd = carry
                t = chunk - 1 - i
                row = pl.ds(pl.multiple_of(t * CH, CH), CH)
                d = [dt[tile[l], row, :] for l in range(lw)]
                du = [ut[tile[l], row, :] for l in range(lw)]
                gs = [gt[tile[l], row, :] for l in range(lw)]
                later = pl.ds(pl.multiple_of(t * CH + CH, CH), CH)
                ko, gdo = [], []
                s1 = [None] * lw
                s2 = [None] * lw
                for n in range(ng):
                    w = wx[n, row, :]
                    r = rx[n, row, :]
                    gwn = grn = None
                    for l in range(lw):
                        col = n * lw + l
                        gh = k[n * lw + l] + r * gs[l]
                        kn = ab[col, row, :] * gh
                        q_ = kn * hb[col, row, :]
                        ko.append(kn)
                        gdo.append(gd[n * lw + l] + q_ * d[l])
                        f1 = rate[n][l] * q_
                        f2 = gh * w
                        s1[l] = f1 if n == 0 else s1[l] + f1
                        s2[l] = f2 if n == 0 else s2[l] + f2
                        gwn = gh * du[l] if l == 0 else gwn + gh * du[l]
                        hr = gs[l] * hb[col, later, :]
                        grn = hr if l == 0 else grn + hr
                    gw[n, row, :] = gwn if q == 0 else gw[n, row, :] + gwn
                    gr[n, row, :] = grn if q == 0 else gr[n, row, :] + grn
                for l in range(lw):
                    s1t[tile[l], row, :] = s1[l] if g == 0 else s1t[tile[l], row, :] + s1[l]
                    s2t[tile[l], row, :] = s2[l] if g == 0 else s2t[tile[l], row, :] + s2[l]
                return tuple(ko), tuple(gdo)

            unused, gd = _split_loop(chunk, 2, final, (tuple(begin_at), (zero,) * (ng * lw)), 2, point)
            for n in range(ng):
                for l in range(lw):
                    gd_ref[g * ng + n : g * ng + n + 1, lanes[l]] = jnp.sum(gd[n * lw + l], axis=0, keepdims=True)

        c_at = lax.broadcasted_iota(jnp.int32, (2 * state, 128), 0)
        for c in range(CH):
            rows = pl.ds(c, chunk, stride=CH)
            here = slice(c * chunk, (c + 1) * chunk)
            part = None if g == 0 else gwr_ref[:, here]
            for n in range(ng):
                for src, base in ((gw, 0), (gr, state)):
                    ones = jnp.where(c_at == base + g * ng + n, 1.0, 0.0).astype(BF)
                    one = lax.dot_general(
                        ones,
                        src.at[n][rows, :].astype(BF),
                        (((1,), (1,)), ((), ())),
                        preferred_element_type=F32,
                    )
                    part = one if part is None else part + one
            gwr_ref[:, here] = part
    while todo:
        point()
    _unweave(s1_ref, s1t, chunk)
    _unweave(s2_ref, s2t, chunk)
    if hide:
        finish()


def scan_bwd(delta, inner, gs, pick, a2, hin, k0, rank, state, part=None):
    length, el = delta.shape
    chunk = length // CH
    lw = min(4, el // 128)
    ng = 4 if lw == 4 else 8
    f32 = F32
    vmem = pl.BlockSpec(memory_space=pltpu.VMEM)
    out_shape = [
        jax.ShapeDtypeStruct((length, el), f32),
        jax.ShapeDtypeStruct((length, el), f32),
        jax.ShapeDtypeStruct((state, el), f32),
        jax.ShapeDtypeStruct((2 * state, length), f32),
        jax.ShapeDtypeStruct((state, el), f32),
    ]
    scratch = (
        [pltpu.VMEM((ng, length, 128), f32)] * 4
        + [pltpu.VMEM((ng * lw, length, 128), f32), pltpu.VMEM((ng * lw, length + CH, 128), f32)]
        + [pltpu.VMEM((el // 128, length, 128), f32)] * 5
    )
    args = [delta, inner, gs, pick, a2, hin, k0]
    params = dict(vmem_limit_bytes=67043328)
    if part is not None:
        args.append(part)
        out_shape.append(jax.ShapeDtypeStruct((part.shape[0] // 8, part.shape[1]), f32))
        scratch += scatter_scratch(part.shape[0] // 8, part.shape[1], 2)
        params.update(collective_id=6, has_side_effects=True)
    return pl.pallas_call(
        functools.partial(bwd_kernel, chunk, lw, ng, rank, state, 0 if part is None else 1),
        out_shape=tuple(out_shape),
        in_specs=[vmem] * len(args),
        out_specs=tuple([vmem] * len(out_shape)),
        scratch_shapes=scratch,
        compiler_params=pltpu.CompilerParams(**params),
        name="scan_bwd",
    )(*args)


EPS = 1e-05
LN2 = 0.6931471805599453
SEGMENT = 1024


def peers_barrier(seq_peers, dp_peers):
    barrier = pltpu.get_barrier_semaphore()
    for p in seq_peers:
        pl.semaphore_signal(barrier, inc=1, device_id={"seq": p}, device_id_type=MESH)
    for p in dp_peers:
        pl.semaphore_signal(barrier, inc=1, device_id={"dp": p}, device_id_type=MESH)
    pl.semaphore_wait(barrier, len(seq_peers) + len(dp_peers))


def sum_kernel(n, part_ref, out_ref, recv, send_sem, recv_sem, back_send, back_recv):
    me = lax.axis_index("seq")
    peers = [lax.rem(me + k, n) for k in range(1, n)]
    peers_barrier(peers, [])

    def at(p):
        return pl.ds(pl.multiple_of(p * 128, 128), 128)

    out = [
        pltpu.make_async_remote_copy(
            src_ref=part_ref.at[:, at(p)],
            dst_ref=recv.at[k],
            send_sem=send_sem.at[k],
            recv_sem=recv_sem.at[k],
            device_id={"seq": p},
            device_id_type=MESH,
        )
        for k, p in enumerate(peers)
    ]
    for c in out:
        c.start()
    total = part_ref[:, at(me)].astype(F32)
    for k, c in enumerate(out):
        c.wait_recv()
        total = total + recv[k].astype(F32)
    out_ref[:, at(me)] = total.astype(BF)
    back = [
        pltpu.make_async_remote_copy(
            src_ref=out_ref.at[:, at(me)],
            dst_ref=out_ref.at[:, at(me)],
            send_sem=back_send.at[k],
            recv_sem=back_recv.at[k],
            device_id={"seq": p},
            device_id_type=MESH,
        )
        for k, p in enumerate(peers)
    ]
    for c in back:
        c.start()
    for c in out:
        c.wait_send()
    for c in back:
        c.wait()


def sum_over_seq(part, n, name, ident):
    rows, length = part.shape
    return pl.pallas_call(
        functools.partial(sum_kernel, n),
        out_shape=jax.ShapeDtypeStruct((rows, length), BF),
        in_specs=[pl.BlockSpec(memory_space=pltpu.VMEM)],
        out_specs=pl.BlockSpec(memory_space=pltpu.VMEM),
        scratch_shapes=[pltpu.VMEM((n - 1, rows, 128), BF)] + [pltpu.SemaphoreType.DMA((n - 1,))] * 4,
        compiler_params=pltpu.CompilerParams(collective_id=ident, has_side_effects=True),
        name=name,
    )(part)


SLAB = 32


def remote(src, dst, ss, rs, to):
    return pltpu.make_async_remote_copy(
        src_ref=src, dst_ref=dst, send_sem=ss, recv_sem=rs, device_id=to, device_id_type=MESH
    )


def gather_stages(xn, xg, z_send, z_recv, y_send, y_recv):
    s = lax.axis_index("seq")
    z, y = s // 2, lax.rem(s, 2)
    other = s + 1 - 2 * y
    col = xn.shape[0] // SLAB
    chains = [(c, y) for c in range(col)] + [(col - 1, 1 - y)]

    def slab(c):
        return pl.ds(c * SLAB, SLAB)

    def z_copy(chain, up, j):
        c, yy = chains[chain]
        block = (z - j if up else z + j) * 2 + yy
        src = xn.at[slab(c)] if (j == 0 and chain < col) else xg.at[block, slab(c)]
        at = chain * 6 + (0 if up else 3) + j
        return remote(src, xg.at[block, slab(c)], z_send.at[at], z_recv.at[at], {"seq": s + 2 if up else s - 2})

    def z_arrived(chain, up, j):
        c, yy = chains[chain]
        block = (z - j if up else z + j) * 2 + yy
        at = chain * 6 + (0 if up else 3) + j - 1
        ref = xg.at[block, slab(c)]
        return remote(ref, ref, z_send.at[at], z_recv.at[at], {"seq": s})

    def can(up, j):
        return z >= j if up else z <= 3 - j

    def can_send(up):
        return z < 3 if up else z > 0

    def y_copy(chain, where):
        c = chains[chain][0]
        block = (z + where) * 2 + y
        src = xn.at[slab(c)] if where == 0 else xg.at[block, slab(c)]
        at = chain * 7 + where + 3
        return remote(src, xg.at[block, slab(c)], y_send.at[at], y_recv.at[at], {"seq": other})

    def y_arrived(chain, where):
        c = chains[chain][0]
        ref = xg.at[(z + where) * 2 + 1 - y, slab(c)]
        at = chain * 7 + where + 3
        return remote(ref, ref, y_send.at[at], y_recv.at[at], {"seq": s})

    def start():
        y_copy(col - 1, 0).start()
        for chain in [col - 1] + list(range(col - 1)):
            for up in (True, False):

                @pl.when(can_send(up))
                def _():
                    z_copy(chain, up, 0).start()

            if chain < col - 1:
                y_copy(chain, 0).start()

    def cross_over():
        y_arrived(col - 1, 0).wait_recv()
        for up in (True, False):

            @pl.when(can_send(up))
            def _():
                z_copy(col, up, 0).start()

    def relay(j, chain):
        for up in (True, False):

            @pl.when(can(up, j))
            def _():
                z_arrived(chain, up, j).wait_recv()
                if j < 3:

                    @pl.when(can_send(up))
                    def _():
                        z_copy(chain, up, j).start()

                if chain < col - 1:
                    y_copy(chain, -j if up else j).start()

    def z_round(j):
        for chain in [col - 1] + list(range(col - 1)) + [col]:
            relay(j, chain)

    def finish():
        for chain in range(col - 1):
            y_arrived(chain, 0).wait_recv()
            for j in (1, 2, 3):
                for up in (True, False):

                    @pl.when(can(up, j))
                    def _():
                        y_arrived(chain, -j if up else j).wait_recv()

        y_copy(col - 1, 0).wait_send()
        for chain in range(col - 1):
            y_copy(chain, 0).wait_send()
            for j in (1, 2, 3):
                for up in (True, False):

                    @pl.when(can(up, j))
                    def _():
                        y_copy(chain, -j if up else j).wait_send()

        for chain in range(col + 1):
            for up in (True, False):

                @pl.when(can_send(up))
                def _():
                    z_copy(chain, up, 0).wait_send()

                for j in (1, 2):

                    @pl.when(jnp.logical_and(can(up, j), can_send(up)))
                    def _():
                        z_copy(chain, up, j).wait_send()

    steps = [cross_over] + [functools.partial(z_round, j) for j in (1, 2, 3)]
    return start, steps, finish


def gather_sems(rows):
    col = rows // SLAB
    dma = pltpu.SemaphoreType.DMA
    return [dma(((col + 1) * 6,)), dma(((col + 1) * 6,)), dma((col * 7,)), dma((col * 7,))]


def front_kernel(count, *refs):
    xs, refs = refs[:count], refs[count:]
    wp, pk, gn = refs[:3]
    xgs, refs = refs[3 : 3 + count], refs[3 + count :]
    wg, pg, gg = refs[:3]
    local_sem, w_send, w_recv, d_send, d_recv, p_send, p_recv, g_send, g_recv = refs[3:12]
    sems = [refs[12 + 4 * i : 16 + 4 * i] for i in range(count)]
    s = lax.axis_index("seq")
    d = lax.axis_index("dp")
    n = 8
    cross = lax.rem(d + 2, 4)
    core = d + 1 - 2 * lax.rem(d, 2)
    diag = lax.rem(core + 2, 4)
    peers = [lax.rem(s + k, n) for k in range(1, n)]
    sources = [lax.rem(s + n - 1 - k, n) for k in range(n - 1)] + [s]
    peers_barrier(peers, [cross, core])
    col = pk.shape[0] // SLAB
    gathers = [gather_stages(x, xg, *sm) for x, xg, sm in zip(xs, xgs, sems)]
    own = [
        pltpu.make_async_copy(wp.at[s], wg.at[d, s], local_sem.at[0]),
        pltpu.make_async_copy(pk, pg.at[d], local_sem.at[1]),
        pltpu.make_async_copy(gn, gg.at[d, s], local_sem.at[2]),
    ] + [pltpu.make_async_copy(x, xg.at[s], local_sem.at[3 + i]) for i, (x, xg) in enumerate(zip(xs, xgs))]

    def slab(c):
        return pl.ds(c * SLAB, SLAB)

    def w_copy(k):
        return remote(wp.at[peers[k]], wg.at[d, s], w_send.at[k], w_recv.at[k], {"seq": peers[k]})

    def g_copy(k):
        return remote(gn, gg.at[d, s], g_send.at[k], g_recv.at[k], {"seq": peers[k]})

    def g_over(kind):
        block = cross if kind == 2 else d
        at = 7 + kind
        return remote(gg.at[block], gg.at[block], g_send.at[at], g_recv.at[at], {"dp": cross if kind == 0 else core})

    def d_copy(k, kind):
        block = cross if kind == 2 else d
        src = wp.at[s] if (k == 7 and kind < 2) else wg.at[block, sources[k]]
        at = k * 3 + kind
        return remote(
            src, wg.at[block, sources[k]], d_send.at[at], d_recv.at[at], {"dp": cross if kind == 0 else core}
        )

    def p_copy(c, kind):
        block = cross if kind == 2 else d
        src = pk.at[slab(c)] if kind < 2 else pg.at[block, slab(c)]
        at = c * 3 + kind
        return remote(src, pg.at[block, slab(c)], p_send.at[at], p_recv.at[at], {"dp": cross if kind == 0 else core})

    def arrived(ref, sem_s, sem_r):
        remote(ref, ref, sem_s, sem_r, {"seq": s}).wait_recv()

    def w_relay(k):
        arrived(wg.at[d, sources[k]], w_send.at[k], w_recv.at[k])
        for kind in (0, 1):
            d_copy(k, kind).start()

    def cross_relay(k):
        arrived(wg.at[cross, sources[k]], d_send.at[k * 3], d_recv.at[k * 3])
        d_copy(k, 2).start()

    for k in range(n - 1):
        g_copy(k).start()
    for k in range(n - 1):
        w_copy(k).start()
    gathers[0][0]()
    for kind in (0, 1):
        d_copy(7, kind).start()
    for c in range(col):
        for kind in (0, 1):
            p_copy(c, kind).start()
    for c in own:
        c.start()
    own[2].wait()
    for k in range(n - 1):
        arrived(gg.at[d, sources[k]], g_send.at[k], g_recv.at[k])
    for kind in (0, 1):
        g_over(kind).start()
    steps = gathers[0][1]
    steps[0]()
    steps[1]()
    for k in (0, 1, 5, 6):
        w_relay(k)
    arrived(gg.at[cross], g_send.at[7], g_recv.at[7])
    g_over(2).start()
    steps[2]()
    for k in (2, 3, 4):
        w_relay(k)
    for c in range(col):
        arrived(pg.at[cross, slab(c)], p_send.at[c * 3], p_recv.at[c * 3])
        p_copy(c, 2).start()
    steps[3]()
    for extra in gathers[1:]:
        extra[0]()
    for k in (7, 0, 1, 5, 6, 2, 3, 4):
        cross_relay(k)
    gathers[0][2]()
    for extra in gathers[1:]:
        for st in extra[1]:
            st()
        extra[2]()
    for k in range(n):
        for kind, block in ((1, core), (2, diag)):
            at = k * 3 + kind
            arrived(wg.at[block, sources[k]], d_send.at[at], d_recv.at[at])
    for c in range(col):
        for kind, block in ((1, core), (2, diag)):
            at = c * 3 + kind
            arrived(pg.at[block, slab(c)], p_send.at[at], p_recv.at[at])
    for kind, block in ((1, core), (2, diag)):
        arrived(gg.at[block], g_send.at[7 + kind], g_recv.at[7 + kind])
    for k in range(n - 1):
        w_copy(k).wait_send()
        g_copy(k).wait_send()
    for kind in (0, 1, 2):
        g_over(kind).wait_send()
        for k in range(n):
            d_copy(k, kind).wait_send()
        for c in range(col):
            p_copy(c, kind).wait_send()
    for i, c in enumerate(own):
        if i != 2:
            c.wait()


def front_gather(xs, wp, pk, gn):
    col = pk.shape[0] // SLAB
    count = len(xs)
    dma = pltpu.SemaphoreType.DMA
    scratch = [dma((3 + count,)), dma((7,)), dma((7,)), dma((24,)), dma((24,)), dma((col * 3,)), dma((col * 3,)), dma((10,)), dma((10,))]
    for x in xs:
        scratch += gather_sems(x.shape[0])
    return pl.pallas_call(
        functools.partial(front_kernel, count),
        out_shape=tuple(jax.ShapeDtypeStruct((8,) + x.shape, BF) for x in xs)
        + (
            jax.ShapeDtypeStruct((4,) + wp.shape, BF),
            jax.ShapeDtypeStruct((4,) + pk.shape, BF),
            jax.ShapeDtypeStruct((4, 8) + gn.shape, gn.dtype),
        ),
        in_specs=[pl.BlockSpec(memory_space=pltpu.VMEM)] * (count + 3),
        out_specs=tuple([pl.BlockSpec(memory_space=pl.ANY)] * (count + 3)),
        scratch_shapes=scratch,
        compiler_params=pltpu.CompilerParams(
            collective_id=3, has_side_effects=True, vmem_limit_bytes=60 << 20
        ),
        name="front_gather",
    )(*xs, wp, pk, gn)


def add_blocks(dst, srcs):
    rows = dst.shape[0]
    width = dst.shape[1]
    step = 16 if rows % 16 == 0 else rows

    @pl.loop(0, rows // step)
    def _(i):
        at = pl.ds(pl.multiple_of(i * step, step), step)
        total = srcs[0][at, :].astype(F32)
        for s_ref in srcs[1:]:
            total = total + s_ref[at, :].astype(F32)
        dst[at, :] = total.astype(dst.dtype)


def scatter_stages(part, out, ybuf, zbuf, sbuf, qbuf, y_send, y_recv, z_send, z_recv, q_send, q_recv):
    s = lax.axis_index("seq")
    z, y = s // 2, lax.rem(s, 2)
    other = s + 1 - 2 * y
    rows = out.shape[0]
    slabs = rows // SLAB
    np_ = ybuf.shape[1]
    items = [(c, own, False) for c in range(np_, slabs) for own in (True, False)] + [(c, True, True) for c in range(np_)]

    def own_part(zz, yy, c):
        return part.at[pl.ds(pl.multiple_of((zz * 2 + yy) * rows + c * SLAB, SLAB), SLAB), :]

    def y_at(k):
        return jnp.where(z < 2, 3 - k, k)

    def y_copy(c, k):
        zz = y_at(k)
        at = c * 4 + k
        return remote(own_part(zz, 1 - y, c), ybuf.at[zz, c], y_send.at[at], y_recv.at[at], {"seq": other})

    def base(i, zz):
        c, own, crossed = items[i]
        yy = y if own else 1 - y
        refs = [own_part(zz, yy, c)]
        if crossed:
            refs.append(ybuf.at[zz, c])
        return refs

    def z_at(direction, q, i):
        return (direction * 4 + q) * len(items) + i

    def z_copy(direction, h, q, i):
        zz = q if direction == 0 else 3 - q
        refs = base(i, zz)
        src = refs[0] if (h == 0 and len(refs) == 1) else sbuf.at[direction, q - 1, i]
        at = z_at(direction, q, i)
        return remote(
            src, zbuf.at[direction, q - 1, i], z_send.at[at], z_recv.at[at], {"seq": s + 2 if direction == 0 else s - 2}
        )

    def hop(i, h):
        for direction in (0, 1):
            pos = z if direction == 0 else 3 - z

            @pl.when(pos == h)
            def _():
                for q in range(3, h - 1, -1):
                    if h > 0:
                        z_copy(direction, h, q, i).wait_recv()
                    if q > h:
                        zz = q if direction == 0 else 3 - q
                        refs = base(i, zz)
                        if h > 0:
                            refs = refs + [zbuf.at[direction, q - 1, i]]
                        if len(refs) > 1:
                            add_blocks(sbuf.at[direction, q - 1, i], refs)
                        z_copy(direction, h, q, i).start()

    def q_copy(j):
        return remote(qbuf.at[0, j], qbuf.at[1, j], q_send.at[j], q_recv.at[j], {"seq": other})

    def settle(i):
        c, own, crossed = items[i]
        dst = out.at[pl.ds(c * SLAB, SLAB), :] if own else qbuf.at[0, c - np_]
        for low, high in ((True, False), (False, False), (False, True)):
            where = z == 0 if low else (z == 3 if high else jnp.logical_and(z > 0, z < 3))

            @pl.when(where)
            def _():
                refs = base(i, z)
                if not low:
                    refs = refs + [zbuf.at[0, z - 1, i]]
                if not high:
                    refs = refs + [zbuf.at[1, 2 - z, i]]
                add_blocks(dst, refs)

        if not own:
            q_copy(c - np_).start()

    def start():
        for c in range(np_):
            for k in range(4):
                y_copy(c, k).start()

    def y_wait(i):
        c, own, crossed = items[i]
        if crossed:
            for k in range(4):
                y_copy(c, k).wait_recv()

    steps = []
    for tau in range(len(items) + 4):
        group = []
        for i in range(len(items)):
            h = tau - i
            if 0 <= h <= 4:
                group.append((i, h))

        def step(group=group):
            for i, h in group:
                if h == 0:
                    y_wait(i)
                if h < 4:
                    hop(i, h)
                else:
                    settle(i)

        steps.append(step)

    def finish():
        for c in range(np_, slabs):
            q_copy(c - np_).wait_recv()
            dst = out.at[pl.ds(c * SLAB, SLAB), :]
            add_blocks(dst, [dst, qbuf.at[1, c - np_]])
        for c in range(np_, slabs):
            q_copy(c - np_).wait_send()
        for c in range(np_):
            for k in range(4):
                y_copy(c, k).wait_send()
        for i in range(len(items)):
            for direction in (0, 1):
                pos = z if direction == 0 else 3 - z
                for h in range(3):

                    @pl.when(pos == h)
                    def _():
                        for q in range(3, h, -1):
                            z_copy(direction, h, q, i).wait_send()

    return start, steps, finish


def scatter_scratch(rows, width, np_):
    slabs = rows // SLAB
    nq = slabs - np_
    count = 2 * nq + np_
    dma = pltpu.SemaphoreType.DMA
    return [
        pltpu.VMEM((4, np_, SLAB, width), BF),
        pltpu.VMEM((2, 3, count, SLAB, width), BF),
        pltpu.VMEM((2, 3, count, SLAB, width), BF),
        pltpu.VMEM((2, nq, SLAB, width), BF),
        dma((4 * np_,)),
        dma((4 * np_,)),
        dma((8 * count,)),
        dma((8 * count,)),
        dma((nq,)),
        dma((nq,)),
    ]


def reduce_stages(src, cbuf, abuf, xbuf, c_send, c_recv, x_send, x_recv, blocks, order, settle):
    d = lax.axis_index("dp")
    cross = lax.rem(d + 2, 4)
    core = d + 1 - 2 * lax.rem(d, 2)
    diag = lax.rem(core + 2, 4)

    def c_copy(kind, b):
        at = kind * blocks + b
        return remote(src(diag if kind else core, order(b)), cbuf.at[kind, b], c_send.at[at], c_recv.at[at], {"dp": core})

    def x_copy(b):
        return remote(abuf.at[b], xbuf.at[b], x_send.at[b], x_recv.at[b], {"dp": cross})

    def start():
        for kind in (1, 0):
            for b in range(blocks):
                c_copy(kind, b).start()

    def first(b):
        c_copy(1, b).wait_recv()
        add_blocks(abuf.at[b], [src(cross, order(b)), cbuf.at[1, b]])
        x_copy(b).start()

    def second(b):
        c_copy(0, b).wait_recv()
        x_copy(b).wait_recv()
        settle(b, [src(d, order(b)), cbuf.at[0, b], xbuf.at[b]])

    def finish():
        for b in range(blocks):
            for kind in (0, 1):
                c_copy(kind, b).wait_send()
            x_copy(b).wait_send()

    return start, first, second, finish


def reduce_scratch(blocks, rows, width):
    dma = pltpu.SemaphoreType.DMA
    return [
        pltpu.VMEM((2, blocks, rows, width), BF),
        pltpu.VMEM((blocks, rows, width), BF),
        pltpu.VMEM((blocks, rows, width), BF),
        dma((2 * blocks,)),
        dma((2 * blocks,)),
        dma((blocks,)),
        dma((blocks,)),
    ]


def tail_kernel(count, n_pack, *refs):
    parts, refs = refs[:count], refs[count:]
    g, refs = refs[0], refs[1:]
    pg, refs = (refs[0], refs[1:]) if n_pack else (None, refs)
    outs, refs = refs[:count], refs[count:]
    gout, refs = refs[0], refs[1:]
    pout, refs = (refs[0], refs[1:]) if n_pack else (None, refs)
    scat = [refs[i * 10 : i * 10 + 10] for i in range(count)]
    refs = refs[10 * count :]
    red, refs = refs[:7], refs[7:]
    packed_red, refs = (refs[:7], refs[7:]) if n_pack else (None, refs)
    fbuf, f_send, f_recv = refs
    s = lax.axis_index("seq")
    d = lax.axis_index("dp")
    n = 8
    peers = [lax.rem(s + k, n) for k in range(1, n)]
    peers_barrier(peers, [lax.rem(d + 2, 4), d + 1 - 2 * lax.rem(d, 2)])

    def order(b):
        return lax.rem(s + b, n)

    def f_copy(b):
        return remote(fbuf.at[b - 1], gout.at[s], f_send.at[b - 1], f_recv.at[b - 1], {"seq": order(b)})

    def f_settle(b, srcs):
        if b == 0:
            add_blocks(gout.at[s], srcs)
        else:
            add_blocks(fbuf.at[b - 1], srcs)
            f_copy(b).start()

    scatters = [scatter_stages(p, o, *sc) for p, o, sc in zip(parts, outs, scat)]
    start, first, second, finish = reduce_stages(lambda dd, b: g.at[dd, b], *red, n, order, f_settle)
    for sc in scatters:
        sc[0]()
    start()
    if n_pack:

        def p_settle(b, srcs):
            add_blocks(pout.at[pl.ds(b * SLAB, SLAB), :], srcs)

        p_start, p_first, p_second, p_finish = reduce_stages(
            lambda dd, b: pg.at[dd, pl.ds(b * SLAB, SLAB), :], *packed_red, n_pack, lambda b: b, p_settle
        )
        p_start()
    blocks = [4, 3, 5, 2, 6, 1, 7, 0]
    todo = []
    for b in blocks:
        todo.append(lambda b=b: first(b))
    if n_pack:
        for b in range(n_pack):
            todo.append(lambda b=b: p_first(b))
    seconds = [lambda b=b: second(b) for b in blocks]
    if n_pack:
        seconds = seconds + [lambda b=b: p_second(b) for b in range(n_pack)]
    steps = [st for group in zip(*[sc[1] for sc in scatters]) for st in group]
    if steps:
        steps.pop(0)()
    for t in todo:
        t()
    while steps or seconds:
        if steps:
            steps.pop(0)()
        if seconds:
            seconds.pop(0)()
    for sc in scatters:
        sc[2]()
    for b in range(1, n):
        f_copy(b).wait()
    finish()
    if n_pack:
        p_finish()


def tail_scatter(parts, g, pg, np_):
    rows, width = parts[0].shape[0] // 8 if parts else 0, parts[0].shape[1] if parts else 0
    count = len(parts)
    n_pack = 0 if pg is None else pg.shape[1] // SLAB
    out_shape = [jax.ShapeDtypeStruct((rows, width), F32)] * count + [jax.ShapeDtypeStruct(g.shape[1:], BF)]
    scratch = []
    for _ in range(count):
        scratch += scatter_scratch(rows, width, np_)
    scratch += reduce_scratch(8, g.shape[2], g.shape[3])
    args = list(parts) + [g]
    if n_pack:
        out_shape.append(jax.ShapeDtypeStruct(pg.shape[1:], F32))
        scratch += reduce_scratch(n_pack, SLAB, pg.shape[2])
        args.append(pg)
    scratch += [pltpu.VMEM((7,) + g.shape[2:], BF), pltpu.SemaphoreType.DMA((7,)), pltpu.SemaphoreType.DMA((7,))]
    return pl.pallas_call(
        functools.partial(tail_kernel, count, n_pack),
        out_shape=tuple(out_shape),
        in_specs=[pl.BlockSpec(memory_space=pltpu.VMEM)] * len(args),
        out_specs=tuple([pl.BlockSpec(memory_space=pltpu.VMEM)] * len(out_shape)),
        scratch_shapes=scratch,
        compiler_params=pltpu.CompilerParams(
            collective_id=4, has_side_effects=True, vmem_limit_bytes=63 << 20
        ),
        name="tail_scatter",
    )(*args)


def silu_slope(values_in):
    sigmoid_value = jax.nn.sigmoid(values_in)
    return sigmoid_value * (1.0 + values_in * (1.0 - sigmoid_value))


def dot(a, b, dims):
    return lax.dot_general(a, b, (dims, ((), ())), preferred_element_type=F32)


def segments(length):
    count = max(1, length // SEGMENT)
    size = length // count
    return [(i * size, (i + 1) * size) for i in range(count)]


def forward_scan(step_size, inner, picked, rate2, shard):
    state = rate2.shape[0]
    carry = jnp.zeros(rate2.shape, F32)
    outs, starts = [], []
    for lo, hi in segments(step_size.shape[0]):
        y, start, carry, *gathered = scan_fwd(
            step_size[lo:hi], inner[lo:hi], picked[:, lo:hi], rate2, carry, RANK, state, shard
        )
        outs.append(y)
        starts.append(start)
    return (outs[0] if len(outs) == 1 else jnp.concatenate(outs, axis=0)), starts, gathered


def backward_scan(step_size, inner, grad_scan, picked, rate2, starts, part):
    state = rate2.shape[0]
    carry = jnp.zeros(rate2.shape, F32)
    parts = []
    total = jnp.zeros(rate2.shape, F32)
    spans = segments(step_size.shape[0])
    for (lo, hi), start in reversed(list(zip(spans, starts))):
        s1, s2, decay, gwr, carry, *summed = scan_bwd(
            step_size[lo:hi], inner[lo:hi], grad_scan[lo:hi], picked[:, lo:hi], rate2, start, carry, RANK, state, part
        )
        total = total + decay
        parts.append((s1, s2, gwr))
    parts = parts[::-1]
    if len(parts) == 1:
        s1, s2, gwr = parts[0]
    else:
        s1, s2, gwr = (jnp.concatenate(p, axis=k) for k, p in zip((0, 0, 1), zip(*parts)))
    return s1, s2, gwr, total, summed


def shards(
    block_input,
    norm_gain,
    in_weight,
    conv_weight,
    conv_bias,
    select_weight,
    step_weight,
    step_bias,
    decay_log,
    skip_gain,
    out_weight,
    output_grad,
):
    n_dp, n_seq = lax.axis_size("dp"), lax.axis_size("seq")
    token_rows = block_input[0]
    upstream_rows = output_grad[0]
    width = token_rows.shape[1]
    d_rows = in_weight.shape[0]
    e_rows = out_weight.shape[0]
    local = n_dp * e_rows

    own = token_rows.astype(F32)
    own_scale = lax.rsqrt(jnp.mean(own * own, axis=1, keepdims=True) + EPS)
    pieces = in_weight
    pieces = pieces.reshape(d_rows, 2, n_dp, n_seq, e_rows).transpose(3, 0, 1, 2, 4).reshape(n_seq, d_rows, 2 * local)

    smalls = [select_weight, step_weight, decay_log, conv_weight, conv_bias[:, None], step_bias[:, None], skip_gain[:, None]]
    used = sum(s.shape[1] for s in smalls)
    pad = -used % 128
    packed = jnp.concatenate([out_weight] + smalls + [jnp.zeros((e_rows, pad), BF)], axis=1)
    kernels = (n_dp, n_seq) == (4, 8)
    hide = kernels and HIDE
    if kernels:
        gain_tile = jnp.broadcast_to(jnp.pad(norm_gain.astype(F32), (0, 128 - d_rows))[None], (8, 128))
        *gathered, in_w, packed, gains = front_gather(
            [token_rows] if hide else [token_rows, upstream_rows], pieces, packed, gain_tile
        )
        x = gathered[0]
        packed = packed.reshape(local, packed.shape[2])
        gain = gains[:, :, 0, :d_rows].reshape(width)
    else:
        x = lax.all_gather(token_rows, "seq")
        gathered = [x, lax.all_gather(upstream_rows, "seq")]
        in_w = lax.all_gather(lax.all_to_all(pieces, "seq", 0, 0), "dp")
        packed = lax.all_gather(packed, "dp", axis=0, tiled=True)
        gain = lax.all_gather(norm_gain, ("dp", "seq"), axis=0, tiled=True).astype(F32)
    length = n_seq * token_rows.shape[0]
    in_w = in_w.reshape(width, 2 * local)
    xf = x.reshape(length, width).astype(F32)
    row_scale = lax.rsqrt(jnp.mean(xf * xf, axis=1, keepdims=True) + EPS)
    normed = (xf * row_scale * gain).astype(BF)
    cuts = []
    begin = 0
    for s in [out_weight] + smalls:
        cuts.append((begin, begin + s.shape[1]))
        begin += s.shape[1]
    out_w, sel_w, step_w, dec_w, conv_w, conv_b, step_b, skip = (packed[:, a:b] for a, b in cuts)
    conv_taps = conv_w.astype(F32).T
    conv_b, step_b, skip = (v[:, 0].astype(F32) for v in (conv_b, step_b, skip))
    decay_rate = -jnp.exp(dec_w.astype(F32).T)
    rate2 = decay_rate * (1.0 / LN2)

    mixed = dot(normed, in_w, ((1,), (0,))).astype(BF)
    padded = jnp.concatenate([jnp.zeros((KERNEL - 1, local), BF), mixed[:, :local]], axis=0).astype(F32)
    gate_in = mixed[:, local:].astype(F32)
    conv_out = conv_b + jnp.zeros((length, local), F32)
    for offset in range(KERNEL):
        conv_out = conv_out + padded[offset : offset + length] * conv_taps[offset]
    inner = jax.nn.silu(conv_out).astype(BF)
    inner_f = inner.astype(F32)
    picked = sum_over_seq(dot(sel_w, inner, ((0,), (1,))).astype(BF), n_seq, "sum_picked", 1)
    step_in = picked[:RANK]
    step_raw = dot(step_in, step_w, ((0,), (1,))) + step_b
    step_size = jax.nn.softplus(step_raw)
    scanned, starts, more = forward_scan(step_size, inner_f, picked, rate2, upstream_rows if hide else None)
    mamba_out = scanned + skip * inner_f
    gate_act = jax.nn.silu(gate_in)
    gated_out = (mamba_out * gate_act).astype(BF)
    out_part = dot(gated_out, out_w, ((1,), (0,))).astype(BF)

    upstream = (more[0] if hide else gathered[1]).reshape(length, width)
    grad_gated = dot(upstream, out_w, ((1,), (1,)))
    grad_out_w = dot(gated_out, upstream, ((0,), (0,)))
    grad_scan = grad_gated * gate_act
    grad_gate = grad_gated * mamba_out * silu_slope(gate_in)
    grad_skip = jnp.sum(grad_scan * inner_f, axis=0)
    s1, s2, grad_wr, grad_decay, more = backward_scan(
        step_size, inner_f, grad_scan, picked, rate2, starts, out_part if hide else None
    )
    grad_raw_f = (s1 * LN2 + inner_f * s2) * jax.nn.sigmoid(step_raw)
    grad_step_b = jnp.sum(grad_raw_f, axis=0)
    grad_raw = grad_raw_f.astype(BF)
    grad_step_w = dot(grad_raw, step_in, ((0,), (1,)))
    part = jnp.concatenate([dot(step_w, grad_raw, ((0,), (1,))), grad_wr], axis=0).astype(BF)
    grad_picked = sum_over_seq(part, n_seq, "sum_grad_picked", 2)
    grad_sel = dot(inner, grad_picked, ((0,), (1,)))
    grad_inner = step_size * s2 + grad_scan * skip + dot(grad_picked, sel_w, ((0,), (1,)))
    grad_conv = grad_inner * silu_slope(conv_out)
    grad_conv_b = jnp.sum(grad_conv, axis=0)
    grad_taps = [jnp.sum(grad_conv * padded[k : k + length], axis=0) for k in range(KERNEL)]
    extended = jnp.concatenate([grad_conv, jnp.zeros((KERNEL - 1, local), F32)], axis=0)
    grad_conv_in = jnp.zeros((length, local), F32)
    for k in range(KERNEL):
        grad_conv_in = grad_conv_in + extended[KERNEL - 1 - k : KERNEL - 1 - k + length] * conv_taps[k]
    grad_mixed = jnp.concatenate([grad_conv_in, grad_gate], axis=1).astype(BF)
    grad_in_w = dot(normed, grad_mixed, ((0,), (0,)))
    grad_normed = dot(grad_mixed, in_w, ((1,), (1,)))

    small_grads = [grad_sel, grad_step_w, (grad_decay * decay_rate).T, jnp.stack(grad_taps, axis=1), grad_conv_b[:, None], grad_step_b[:, None], grad_skip[:, None]]
    packed_grad = jnp.concatenate([grad_out_w] + small_grads + [jnp.zeros((local, pad), F32)], axis=1).astype(BF)
    grad_in_w = grad_in_w.astype(BF)
    grad_normed = grad_normed.astype(BF)
    if kernels:
        parts = [grad_normed] if hide else [grad_normed, out_part]
        *summed, grad_in_all, packed_grad = tail_scatter(
            parts,
            grad_in_w.reshape(n_dp, n_seq, d_rows, 2 * local),
            packed_grad.reshape(n_dp, e_rows, packed_grad.shape[1]),
            2,
        )
        grad_normed = summed[0]
        out_rows = more[0] if hide else summed[1]
    else:
        packed_grad = lax.psum_scatter(packed_grad, "dp", scatter_dimension=0, tiled=True).astype(F32)
        grad_in_all = lax.psum_scatter(grad_in_w, "dp", scatter_dimension=0, tiled=True)
        grad_in_all = lax.all_to_all(grad_in_all, "seq", split_axis=0, concat_axis=0, tiled=True)
        grad_in_all = grad_in_all.reshape(n_seq, d_rows, 2 * local)
        grad_normed = lax.psum_scatter(grad_normed, "seq", scatter_dimension=0, tiled=True).astype(F32)
        out_rows = lax.psum_scatter(out_part, "seq", scatter_dimension=0, tiled=True)
    layer_out = (own + out_rows.astype(F32)).astype(BF)
    g_out, g_sel, g_step, g_dec, g_conv, g_cb, g_sb, g_skip = (packed_grad[:, a:b] for a, b in cuts)
    g_in = (
        grad_in_all.reshape(n_seq, d_rows, 2, n_dp, e_rows)
        .transpose(1, 2, 3, 0, 4)
        .reshape(in_weight.shape)
        .astype(F32)
    )
    g_gain = jnp.sum(g_in * in_weight.astype(F32), axis=1) / norm_gain.astype(F32)

    scaled = grad_normed * gain
    grad_rows = own_scale * scaled - own * (own_scale * own_scale * own_scale) * jnp.mean(scaled * own, axis=1, keepdims=True)
    input_grad = (upstream_rows.astype(F32) + grad_rows).astype(BF)
    return (
        layer_out[None],
        input_grad[None],
        g_gain,
        g_in,
        g_conv,
        g_cb[:, 0],
        g_sel,
        g_step,
        g_sb[:, 0],
        g_dec,
        g_skip[:, 0],
        g_out,
    )


def solution(mesh):
    rows = P(("dp", "seq"))
    both = P(("dp", "seq"), None)
    acts = P("dp", "seq", None)
    return jax.shard_map(
        shards,
        mesh=mesh,
        in_specs=(acts, rows, both, both, rows, both, both, rows, both, rows, both, acts),
        out_specs=(acts, acts, rows, both, both, rows, both, both, rows, both, rows, both),
        check_vma=False,
    )
```

```python
import functools
import jax
import jax.numpy as jnp
from jax import lax
from jax.experimental import pallas as pl
from jax.experimental.pallas import tpu as pltpu
from jax.sharding import PartitionSpec as P

RANK = 128
KERNEL = 4
MESH = pl.DeviceIdType.MESH
HIDE = True
BF = jnp.bfloat16
F32 = jnp.float32

CH = 8
BCUTS = (2, 2, 4)
BSPACE = 1
BNP = 3


def _expand(dst, pick_ref, base, first, chunk):
    ng = dst.shape[0]
    cols = pick_ref.shape[0]
    width = ng * 128
    k_at = lax.broadcasted_iota(jnp.int32, (cols, width), 0)
    n_at = lax.broadcasted_iota(jnp.int32, (cols, width), 1) // 128
    pick_one = jnp.where(k_at == base + first + n_at, 1.0, 0.0).astype(BF)
    for c in range(CH):
        tokens = pick_ref[:, c * chunk : (c + 1) * chunk]
        wide = lax.dot_general(
            tokens, pick_one, (((0,), (0,)), ((), ())), preferred_element_type=F32
        )
        for n in range(ng):
            dst.at[n][pl.ds(c, chunk, stride=CH), :] = wide[:, n * 128 : (n + 1) * 128]


def _weave(dst, value, chunk):
    for q in range(dst.shape[0]):
        for c in range(CH):
            dst.at[q][pl.ds(c, chunk, stride=CH), :] = value(
                slice(c * chunk, (c + 1) * chunk), slice(q * 128, (q + 1) * 128)
            )


def _unweave(dst, src, chunk):
    for q in range(src.shape[0]):
        for c in range(CH):
            dst[c * chunk : (c + 1) * chunk, q * 128 : (q + 1) * 128] = src.at[q][
                pl.ds(c, chunk, stride=CH), :
            ]


def _rows_mask(k, up):
    row = lax.broadcasted_iota(jnp.int32, (CH, 128), 0)
    return row < CH - k if up else row >= k


def _link(p, h, up):
    for k in (1, 2, 4):
        mask = _rows_mask(k, up)
        shift = CH - k if up else k
        ps = jnp.where(mask, pltpu.roll(p, shift, 0), 1.0)
        hs = jnp.where(mask, pltpu.roll(h, shift, 0), 0.0)
        h = h + p * hs
        p = p * ps
    return p, h


def _spread(steps, points):
    state = [0, 0]

    def point():
        state[0] += 1
        while state[1] < len(steps) and state[1] * points < state[0] * len(steps):
            steps[state[1]]()
            state[1] += 1

    return point


def _split_loop(total, parts, body, carry, unroll, point):
    size = total // parts
    for i in range(parts):
        carry = lax.fori_loop(i * size, (i + 1) * size, body, carry, unroll=unroll)
        point()
    return carry


def fwd_kernel(chunk, lw, ng, rank, state, hide, *refs):
    delta_ref, inner_ref, pick_ref, a2_ref, h0_ref = refs[:5]
    refs = refs[5:]
    extra_in, refs = refs[:hide], refs[hide:]
    y_ref, hin_ref, hend_ref = refs[:3]
    refs = refs[3:]
    extra_out, refs = refs[:hide], refs[hide:]
    wx, rx, ab, dt, ut, yt = refs[:6]
    groups = (state // ng) * (delta_ref.shape[1] // (128 * lw))
    cuts = 4 if hide else 1
    point = lambda: None
    if hide:
        sems = refs[6:10]
        local_sem = refs[10]
        s = lax.axis_index("seq")
        d = lax.axis_index("dp")
        peers_barrier([lax.rem(s + k, 8) for k in range(1, 8)], [lax.rem(d + 2, 4), d + 1 - 2 * lax.rem(d, 2)])
        start, steps, finish = gather_stages(extra_in[0], extra_out[0], *sems)
        start()
        own = pltpu.make_async_copy(extra_in[0], extra_out[0].at[s], local_sem)
        own.start()
        point = _spread(steps, groups * 2 * cuts)

    el = delta_ref.shape[1]
    _weave(dt, lambda i, j: delta_ref[i, j], chunk)
    _weave(ut, lambda i, j: delta_ref[i, j] * inner_ref[i, j], chunk)
    for g in range(state // ng):
        _expand(wx, pick_ref, rank, g * ng, chunk)
        _expand(rx, pick_ref, rank + state, g * ng, chunk)
        for q in range(el // (128 * lw)):
            tile = [q * lw + l for l in range(lw)]
            lanes = [slice((q * lw + l) * 128, (q * lw + l + 1) * 128) for l in range(lw)]
            rate = [[a2_ref[g * ng + n : g * ng + n + 1, lanes[l]] for l in range(lw)] for n in range(ng)]
            zero = jnp.zeros((CH, 128), F32)

            def first(t, carry):
                h, cum = carry
                row = pl.ds(pl.multiple_of(t * CH, CH), CH)
                d = [dt[tile[l], row, :] for l in range(lw)]
                du = [ut[tile[l], row, :] for l in range(lw)]
                out = []
                for n in range(ng):
                    w = wx[n, row, :]
                    for l in range(lw):
                        a = jnp.exp2(d[l] * rate[n][l])
                        ab[n * lw + l, row, :] = a
                        out.append(a * h[n * lw + l] + w * du[l])
                return tuple(out), tuple(cum[l] + d[l] for l in range(lw))

            h, cum = _split_loop(chunk, cuts, first, ((zero,) * (ng * lw), (zero,) * lw), 4, point)
            begin_at = []
            for n in range(ng):
                for l in range(lw):
                    h0 = h0_ref[g * ng + n : g * ng + n + 1, lanes[l]]
                    p, hh = _link(jnp.exp2(cum[l] * rate[n][l]), h[n * lw + l], False)
                    full = hh + p * h0
                    begin = jnp.where(_rows_mask(1, False), pltpu.roll(full, 1, 0), h0)
                    hin_ref[g * ng + n, :, lanes[l]] = begin
                    hend_ref[g * ng + n : g * ng + n + 1, lanes[l]] = full[CH - 1 : CH]
                    begin_at.append(begin)

            def second(t, h):
                row = pl.ds(pl.multiple_of(t * CH, CH), CH)
                du = [ut[tile[l], row, :] for l in range(lw)]
                out = []
                y = [None] * lw
                for n in range(ng):
                    w = wx[n, row, :]
                    r = rx[n, row, :]
                    for l in range(lw):
                        a = ab[n * lw + l, row, :]
                        hn = a * h[n * lw + l] + w * du[l]
                        out.append(hn)
                        y[l] = r * hn if n == 0 else y[l] + r * hn
                for l in range(lw):
                    yt[tile[l], row, :] = y[l] if g == 0 else yt[tile[l], row, :] + y[l]
                return tuple(out)

            _split_loop(chunk, cuts, second, tuple(begin_at), 4, point)
    _unweave(y_ref, yt, chunk)
    if hide:
        finish()
        own.wait()


def scan_fwd(delta, inner, pick, a2, h0, rank, state, shard=None):
    length, el = delta.shape
    chunk = length // CH
    lw = min(4, el // 128)
    ng = 4 if lw == 4 else 8
    f32 = F32
    vmem = pl.BlockSpec(memory_space=pltpu.VMEM)
    out_shape = [
        jax.ShapeDtypeStruct((length, el), f32),
        jax.ShapeDtypeStruct((state, CH, el), f32),
        jax.ShapeDtypeStruct((state, el), f32),
    ]
    out_specs = [vmem] * 3
    scratch = [
        pltpu.VMEM((ng, length, 128), f32),
        pltpu.VMEM((ng, length, 128), f32),
        pltpu.VMEM((ng * lw, length, 128), f32),
    ] + [pltpu.VMEM((el // 128, length, 128), f32)] * 3
    args = [delta, inner, pick, a2, h0]
    params = dict(vmem_limit_bytes=60 << 20)
    if shard is not None:
        args.append(shard)
        out_shape.append(jax.ShapeDtypeStruct((8,) + shard.shape, BF))
        out_specs.append(pl.BlockSpec(memory_space=pl.ANY))
        scratch += gather_sems(shard.shape[0]) + [pltpu.SemaphoreType.DMA]
        params.update(collective_id=5, has_side_effects=True)
    return pl.pallas_call(
        functools.partial(fwd_kernel, chunk, lw, ng, rank, state, 0 if shard is None else 1),
        out_shape=tuple(out_shape),
        in_specs=[vmem] * len(args),
        out_specs=tuple(out_specs),
        scratch_shapes=scratch,
        compiler_params=pltpu.CompilerParams(**params),
        name="scan_fwd",
    )(*args)


def bwd_kernel(chunk, lw, ng, rank, state, hide, *refs):
    delta_ref, inner_ref, gs_ref, pick_ref, a2_ref, hin_ref, k0_ref = refs[:7]
    refs = refs[7:]
    extra_in, refs = refs[:hide], refs[hide:]
    s1_ref, s2_ref, gd_ref, gwr_ref, kend_ref = refs[:5]
    refs = refs[5:]
    extra_out, refs = refs[:hide], refs[hide:]
    wx, rx, gw, gr, ab, hb, dt, ut, gt, s1t, s2t = refs[:11]
    groups = (state // ng) * (delta_ref.shape[1] // (128 * lw))
    cuts = BCUTS if hide else (1, 1, 1)
    point = lambda: None
    if hide:
        s = lax.axis_index("seq")
        d = lax.axis_index("dp")
        peers_barrier([lax.rem(s + k, 8) for k in range(1, 8)], [lax.rem(d + 2, 4), d + 1 - 2 * lax.rem(d, 2)])
        start, steps, finish = scatter_stages(extra_in[0], extra_out[0], *refs[11:21], spacing=BSPACE)
        start()
        point = _spread(steps, groups * sum(cuts))

    el = delta_ref.shape[1]
    _weave(dt, lambda i, j: delta_ref[i, j], chunk)
    _weave(ut, lambda i, j: delta_ref[i, j] * inner_ref[i, j], chunk)
    _weave(gt, lambda i, j: gs_ref[i, j], chunk)
    for g in range(state // ng):
        _expand(wx, pick_ref, rank, g * ng, chunk)
        _expand(rx, pick_ref, rank + state, g * ng, chunk)
        for q in range(el // (128 * lw)):
            tile = [q * lw + l for l in range(lw)]
            lanes = [slice((q * lw + l) * 128, (q * lw + l + 1) * 128) for l in range(lw)]
            rate = [[a2_ref[g * ng + n : g * ng + n + 1, lanes[l]] for l in range(lw)] for n in range(ng)]
            zero = jnp.zeros((CH, 128), F32)
            begin = []
            for n in range(ng):
                for l in range(lw):
                    h = hin_ref[g * ng + n, :, lanes[l]]
                    hb[n * lw + l, 0:CH, :] = h
                    begin.append(h)

            def ahead(t, carry):
                h, cum = carry
                row = pl.ds(pl.multiple_of(t * CH, CH), CH)
                d = [dt[tile[l], row, :] for l in range(lw)]
                du = [ut[tile[l], row, :] for l in range(lw)]
                later = pl.ds(pl.multiple_of(t * CH + CH, CH), CH)
                out = []
                for n in range(ng):
                    w = wx[n, row, :]
                    for l in range(lw):
                        col = n * lw + l
                        a = jnp.exp2(d[l] * rate[n][l])
                        ab[col, row, :] = a
                        hn = a * h[n * lw + l] + w * du[l]
                        hb[col, later, :] = hn
                        out.append(hn)
                return tuple(out), tuple(cum[l] + d[l] for l in range(lw))

            unused, cum = _split_loop(chunk, cuts[0], ahead, (tuple(begin), (zero,) * lw), 4, point)

            def local(i, k):
                t = chunk - 1 - i
                row = pl.ds(pl.multiple_of(t * CH, CH), CH)
                gs = [gt[tile[l], row, :] for l in range(lw)]
                out = []
                for n in range(ng):
                    r = rx[n, row, :]
                    for l in range(lw):
                        col = n * lw + l
                        out.append(ab[col, row, :] * (k[n * lw + l] + r * gs[l]))
                return tuple(out)

            k = _split_loop(chunk, cuts[1], local, (zero,) * (ng * lw), 4, point)
            begin_at = []
            for n in range(ng):
                for l in range(lw):
                    k0 = k0_ref[g * ng + n : g * ng + n + 1, lanes[l]]
                    p, kk = _link(jnp.exp2(cum[l] * rate[n][l]), k[n * lw + l], True)
                    full = kk + p * k0
                    begin_at.append(jnp.where(_rows_mask(1, True), pltpu.roll(full, CH - 1, 0), k0))
                    kend_ref[g * ng + n : g * ng + n + 1, lanes[l]] = full[0:1]

            def final(i, carry):
                k, gd = carry
                t = chunk - 1 - i
                row = pl.ds(pl.multiple_of(t * CH, CH), CH)
                d = [dt[tile[l], row, :] for l in range(lw)]
                du = [ut[tile[l], row, :] for l in range(lw)]
                gs = [gt[tile[l], row, :] for l in range(lw)]
                later = pl.ds(pl.multiple_of(t * CH + CH, CH), CH)
                ko, gdo = [], []
                s1 = [None] * lw
                s2 = [None] * lw
                for n in range(ng):
                    w = wx[n, row, :]
                    r = rx[n, row, :]
                    gwn = grn = None
                    for l in range(lw):
                        col = n * lw + l
                        gh = k[n * lw + l] + r * gs[l]
                        kn = ab[col, row, :] * gh
                        q_ = kn * hb[col, row, :]
                        ko.append(kn)
                        gdo.append(gd[n * lw + l] + q_ * d[l])
                        f1 = rate[n][l] * q_
                        f2 = gh * w
                        s1[l] = f1 if n == 0 else s1[l] + f1
                        s2[l] = f2 if n == 0 else s2[l] + f2
                        gwn = gh * du[l] if l == 0 else gwn + gh * du[l]
                        hr = gs[l] * hb[col, later, :]
                        grn = hr if l == 0 else grn + hr
                    gw[n, row, :] = gwn if q == 0 else gw[n, row, :] + gwn
                    gr[n, row, :] = grn if q == 0 else gr[n, row, :] + grn
                for l in range(lw):
                    s1t[tile[l], row, :] = s1[l] if g == 0 else s1t[tile[l], row, :] + s1[l]
                    s2t[tile[l], row, :] = s2[l] if g == 0 else s2t[tile[l], row, :] + s2[l]
                return tuple(ko), tuple(gdo)

            unused, gd = _split_loop(chunk, cuts[2], final, (tuple(begin_at), (zero,) * (ng * lw)), 2, point)
            for n in range(ng):
                for l in range(lw):
                    gd_ref[g * ng + n : g * ng + n + 1, lanes[l]] = jnp.sum(gd[n * lw + l], axis=0, keepdims=True)

        c_at = lax.broadcasted_iota(jnp.int32, (2 * state, 128), 0)
        for c in range(CH):
            rows = pl.ds(c, chunk, stride=CH)
            here = slice(c * chunk, (c + 1) * chunk)
            part = None if g == 0 else gwr_ref[:, here]
            for n in range(ng):
                for src, base in ((gw, 0), (gr, state)):
                    ones = jnp.where(c_at == base + g * ng + n, 1.0, 0.0).astype(BF)
                    one = lax.dot_general(
                        ones,
                        src.at[n][rows, :].astype(BF),
                        (((1,), (1,)), ((), ())),
                        preferred_element_type=F32,
                    )
                    part = one if part is None else part + one
            gwr_ref[:, here] = part
    _unweave(s1_ref, s1t, chunk)
    _unweave(s2_ref, s2t, chunk)
    if hide:
        finish()


def scan_bwd(delta, inner, gs, pick, a2, hin, k0, rank, state, part=None):
    length, el = delta.shape
    chunk = length // CH
    lw = min(4, el // 128)
    ng = 4 if lw == 4 else 8
    f32 = F32
    vmem = pl.BlockSpec(memory_space=pltpu.VMEM)
    out_shape = [
        jax.ShapeDtypeStruct((length, el), f32),
        jax.ShapeDtypeStruct((length, el), f32),
        jax.ShapeDtypeStruct((state, el), f32),
        jax.ShapeDtypeStruct((2 * state, length), f32),
        jax.ShapeDtypeStruct((state, el), f32),
    ]
    scratch = (
        [pltpu.VMEM((ng, length, 128), f32)] * 4
        + [pltpu.VMEM((ng * lw, length, 128), f32), pltpu.VMEM((ng * lw, length + CH, 128), f32)]
        + [pltpu.VMEM((el // 128, length, 128), f32)] * 5
    )
    args = [delta, inner, gs, pick, a2, hin, k0]
    params = dict(vmem_limit_bytes=67043328)
    if part is not None:
        args.append(part)
        out_shape.append(jax.ShapeDtypeStruct((part.shape[0] // 8, part.shape[1]), f32))
        scratch += scatter_scratch(part.shape[0] // 8, part.shape[1], BNP)
        params.update(collective_id=6, has_side_effects=True)
    return pl.pallas_call(
        functools.partial(bwd_kernel, chunk, lw, ng, rank, state, 0 if part is None else 1),
        out_shape=tuple(out_shape),
        in_specs=[vmem] * len(args),
        out_specs=tuple([vmem] * len(out_shape)),
        scratch_shapes=scratch,
        compiler_params=pltpu.CompilerParams(**params),
        name="scan_bwd",
    )(*args)


EPS = 1e-05
LN2 = 0.6931471805599453
SEGMENT = 1024


def peers_barrier(seq_peers, dp_peers):
    barrier = pltpu.get_barrier_semaphore()
    for p in seq_peers:
        pl.semaphore_signal(barrier, inc=1, device_id={"seq": p}, device_id_type=MESH)
    for p in dp_peers:
        pl.semaphore_signal(barrier, inc=1, device_id={"dp": p}, device_id_type=MESH)
    pl.semaphore_wait(barrier, len(seq_peers) + len(dp_peers))


def sum_kernel(n, part_ref, out_ref, recv, send_sem, recv_sem, back_send, back_recv):
    me = lax.axis_index("seq")
    peers = [lax.rem(me + k, n) for k in range(1, n)]
    peers_barrier(peers, [])

    def at(p):
        return pl.ds(pl.multiple_of(p * 128, 128), 128)

    out = [
        pltpu.make_async_remote_copy(
            src_ref=part_ref.at[:, at(p)],
            dst_ref=recv.at[k],
            send_sem=send_sem.at[k],
            recv_sem=recv_sem.at[k],
            device_id={"seq": p},
            device_id_type=MESH,
        )
        for k, p in enumerate(peers)
    ]
    for c in out:
        c.start()
    total = part_ref[:, at(me)].astype(F32)
    for k, c in enumerate(out):
        c.wait_recv()
        total = total + recv[k].astype(F32)
    out_ref[:, at(me)] = total.astype(BF)
    back = [
        pltpu.make_async_remote_copy(
            src_ref=out_ref.at[:, at(me)],
            dst_ref=out_ref.at[:, at(me)],
            send_sem=back_send.at[k],
            recv_sem=back_recv.at[k],
            device_id={"seq": p},
            device_id_type=MESH,
        )
        for k, p in enumerate(peers)
    ]
    for c in back:
        c.start()
    for c in out:
        c.wait_send()
    for c in back:
        c.wait()


def sum_over_seq(part, n, name, ident):
    rows, length = part.shape
    return pl.pallas_call(
        functools.partial(sum_kernel, n),
        out_shape=jax.ShapeDtypeStruct((rows, length), BF),
        in_specs=[pl.BlockSpec(memory_space=pltpu.VMEM)],
        out_specs=pl.BlockSpec(memory_space=pltpu.VMEM),
        scratch_shapes=[pltpu.VMEM((n - 1, rows, 128), BF)] + [pltpu.SemaphoreType.DMA((n - 1,))] * 4,
        compiler_params=pltpu.CompilerParams(collective_id=ident, has_side_effects=True),
        name=name,
    )(part)


SLAB = 32


def remote(src, dst, ss, rs, to):
    return pltpu.make_async_remote_copy(
        src_ref=src, dst_ref=dst, send_sem=ss, recv_sem=rs, device_id=to, device_id_type=MESH
    )


def gather_stages(xn, xg, z_send, z_recv, y_send, y_recv):
    s = lax.axis_index("seq")
    z, y = s // 2, lax.rem(s, 2)
    other = s + 1 - 2 * y
    col = xn.shape[0] // SLAB
    chains = [(c, y) for c in range(col)] + [(col - 1, 1 - y)]

    def slab(c):
        return pl.ds(c * SLAB, SLAB)

    def z_copy(chain, up, j):
        c, yy = chains[chain]
        block = (z - j if up else z + j) * 2 + yy
        src = xn.at[slab(c)] if (j == 0 and chain < col) else xg.at[block, slab(c)]
        at = chain * 6 + (0 if up else 3) + j
        return remote(src, xg.at[block, slab(c)], z_send.at[at], z_recv.at[at], {"seq": s + 2 if up else s - 2})

    def z_arrived(chain, up, j):
        c, yy = chains[chain]
        block = (z - j if up else z + j) * 2 + yy
        at = chain * 6 + (0 if up else 3) + j - 1
        ref = xg.at[block, slab(c)]
        return remote(ref, ref, z_send.at[at], z_recv.at[at], {"seq": s})

    def can(up, j):
        return z >= j if up else z <= 3 - j

    def can_send(up):
        return z < 3 if up else z > 0

    def y_copy(chain, where):
        c = chains[chain][0]
        block = (z + where) * 2 + y
        src = xn.at[slab(c)] if where == 0 else xg.at[block, slab(c)]
        at = chain * 7 + where + 3
        return remote(src, xg.at[block, slab(c)], y_send.at[at], y_recv.at[at], {"seq": other})

    def y_arrived(chain, where):
        c = chains[chain][0]
        ref = xg.at[(z + where) * 2 + 1 - y, slab(c)]
        at = chain * 7 + where + 3
        return remote(ref, ref, y_send.at[at], y_recv.at[at], {"seq": s})

    def start():
        y_copy(col - 1, 0).start()
        for chain in [col - 1] + list(range(col - 1)):
            for up in (True, False):

                @pl.when(can_send(up))
                def _():
                    z_copy(chain, up, 0).start()

            if chain < col - 1:
                y_copy(chain, 0).start()

    def cross_over():
        y_arrived(col - 1, 0).wait_recv()
        for up in (True, False):

            @pl.when(can_send(up))
            def _():
                z_copy(col, up, 0).start()

    def relay(j, chain):
        for up in (True, False):

            @pl.when(can(up, j))
            def _():
                z_arrived(chain, up, j).wait_recv()
                if j < 3:

                    @pl.when(can_send(up))
                    def _():
                        z_copy(chain, up, j).start()

                if chain < col - 1:
                    y_copy(chain, -j if up else j).start()

    def finish():
        for chain in range(col - 1):
            y_arrived(chain, 0).wait_recv()
            for j in (1, 2, 3):
                for up in (True, False):

                    @pl.when(can(up, j))
                    def _():
                        y_arrived(chain, -j if up else j).wait_recv()

        y_copy(col - 1, 0).wait_send()
        for chain in range(col - 1):
            y_copy(chain, 0).wait_send()
            for j in (1, 2, 3):
                for up in (True, False):

                    @pl.when(can(up, j))
                    def _():
                        y_copy(chain, -j if up else j).wait_send()

        for chain in range(col + 1):
            for up in (True, False):

                @pl.when(can_send(up))
                def _():
                    z_copy(chain, up, 0).wait_send()

                for j in (1, 2):

                    @pl.when(jnp.logical_and(can(up, j), can_send(up)))
                    def _():
                        z_copy(chain, up, j).wait_send()

    order = [col - 1] + list(range(col - 1)) + [col]
    steps = [cross_over] + [functools.partial(relay, j, chain) for j in (1, 2, 3) for chain in order]
    return start, steps, finish


def gather_sems(rows):
    col = rows // SLAB
    dma = pltpu.SemaphoreType.DMA
    return [dma(((col + 1) * 6,)), dma(((col + 1) * 6,)), dma((col * 7,)), dma((col * 7,))]


def front_kernel(count, *refs):
    xs, refs = refs[:count], refs[count:]
    wp, pk, gn = refs[:3]
    xgs, refs = refs[3 : 3 + count], refs[3 + count :]
    wg, pg, gg = refs[:3]
    local_sem, w_send, w_recv, d_send, d_recv, p_send, p_recv, g_send, g_recv = refs[3:12]
    sems = [refs[12 + 4 * i : 16 + 4 * i] for i in range(count)]
    s = lax.axis_index("seq")
    d = lax.axis_index("dp")
    n = 8
    cross = lax.rem(d + 2, 4)
    core = d + 1 - 2 * lax.rem(d, 2)
    diag = lax.rem(core + 2, 4)
    peers = [lax.rem(s + k, n) for k in range(1, n)]
    sources = [lax.rem(s + n - 1 - k, n) for k in range(n - 1)] + [s]
    peers_barrier(peers, [cross, core])
    col = pk.shape[0] // SLAB
    gathers = [gather_stages(x, xg, *sm) for x, xg, sm in zip(xs, xgs, sems)]
    own = [
        pltpu.make_async_copy(wp.at[s], wg.at[d, s], local_sem.at[0]),
        pltpu.make_async_copy(pk, pg.at[d], local_sem.at[1]),
        pltpu.make_async_copy(gn, gg.at[d, s], local_sem.at[2]),
    ] + [pltpu.make_async_copy(x, xg.at[s], local_sem.at[3 + i]) for i, (x, xg) in enumerate(zip(xs, xgs))]

    def slab(c):
        return pl.ds(c * SLAB, SLAB)

    def w_copy(k):
        return remote(wp.at[peers[k]], wg.at[d, s], w_send.at[k], w_recv.at[k], {"seq": peers[k]})

    def g_copy(k):
        return remote(gn, gg.at[d, s], g_send.at[k], g_recv.at[k], {"seq": peers[k]})

    def g_over(kind):
        block = cross if kind == 2 else d
        at = 7 + kind
        return remote(gg.at[block], gg.at[block], g_send.at[at], g_recv.at[at], {"dp": cross if kind == 0 else core})

    def d_copy(k, kind):
        block = cross if kind == 2 else d
        src = wp.at[s] if (k == 7 and kind < 2) else wg.at[block, sources[k]]
        at = k * 3 + kind
        return remote(
            src, wg.at[block, sources[k]], d_send.at[at], d_recv.at[at], {"dp": cross if kind == 0 else core}
        )

    def p_copy(c, kind):
        block = cross if kind == 2 else d
        src = pk.at[slab(c)] if kind < 2 else pg.at[block, slab(c)]
        at = c * 3 + kind
        return remote(src, pg.at[block, slab(c)], p_send.at[at], p_recv.at[at], {"dp": cross if kind == 0 else core})

    def arrived(ref, sem_s, sem_r):
        remote(ref, ref, sem_s, sem_r, {"seq": s}).wait_recv()

    def w_relay(k):
        arrived(wg.at[d, sources[k]], w_send.at[k], w_recv.at[k])
        for kind in (0, 1):
            d_copy(k, kind).start()

    def cross_relay(k):
        arrived(wg.at[cross, sources[k]], d_send.at[k * 3], d_recv.at[k * 3])
        d_copy(k, 2).start()

    for k in range(n - 1):
        g_copy(k).start()
    for k in range(n - 1):
        w_copy(k).start()
    gathers[0][0]()
    for kind in (0, 1):
        d_copy(7, kind).start()
    for c in range(col):
        for kind in (0, 1):
            p_copy(c, kind).start()
    for c in own:
        c.start()
    own[2].wait()
    for k in range(n - 1):
        arrived(gg.at[d, sources[k]], g_send.at[k], g_recv.at[k])
    for kind in (0, 1):
        g_over(kind).start()
    steps = gathers[0][1]
    count = len(steps) // 3
    for st in steps[: count + 1]:
        st()
    for k in (0, 1, 5, 6):
        w_relay(k)
    arrived(gg.at[cross], g_send.at[7], g_recv.at[7])
    g_over(2).start()
    for st in steps[count + 1 : 2 * count + 1]:
        st()
    for k in (2, 3, 4):
        w_relay(k)
    for c in range(col):
        arrived(pg.at[cross, slab(c)], p_send.at[c * 3], p_recv.at[c * 3])
        p_copy(c, 2).start()
    for st in steps[2 * count + 1 :]:
        st()
    for extra in gathers[1:]:
        extra[0]()
    for k in (7, 0, 1, 5, 6, 2, 3, 4):
        cross_relay(k)
    gathers[0][2]()
    for extra in gathers[1:]:
        for st in extra[1]:
            st()
        extra[2]()
    for k in range(n):
        for kind, block in ((1, core), (2, diag)):
            at = k * 3 + kind
            arrived(wg.at[block, sources[k]], d_send.at[at], d_recv.at[at])
    for c in range(col):
        for kind, block in ((1, core), (2, diag)):
            at = c * 3 + kind
            arrived(pg.at[block, slab(c)], p_send.at[at], p_recv.at[at])
    for kind, block in ((1, core), (2, diag)):
        arrived(gg.at[block], g_send.at[7 + kind], g_recv.at[7 + kind])
    for k in range(n - 1):
        w_copy(k).wait_send()
        g_copy(k).wait_send()
    for kind in (0, 1, 2):
        g_over(kind).wait_send()
        for k in range(n):
            d_copy(k, kind).wait_send()
        for c in range(col):
            p_copy(c, kind).wait_send()
    for i, c in enumerate(own):
        if i != 2:
            c.wait()


def front_gather(xs, wp, pk, gn):
    col = pk.shape[0] // SLAB
    count = len(xs)
    dma = pltpu.SemaphoreType.DMA
    scratch = [dma((3 + count,)), dma((7,)), dma((7,)), dma((24,)), dma((24,)), dma((col * 3,)), dma((col * 3,)), dma((10,)), dma((10,))]
    for x in xs:
        scratch += gather_sems(x.shape[0])
    return pl.pallas_call(
        functools.partial(front_kernel, count),
        out_shape=tuple(jax.ShapeDtypeStruct((8,) + x.shape, BF) for x in xs)
        + (
            jax.ShapeDtypeStruct((4,) + wp.shape, BF),
            jax.ShapeDtypeStruct((4,) + pk.shape, BF),
            jax.ShapeDtypeStruct((4, 8) + gn.shape, gn.dtype),
        ),
        in_specs=[pl.BlockSpec(memory_space=pltpu.VMEM)] * (count + 3),
        out_specs=tuple([pl.BlockSpec(memory_space=pl.ANY)] * (count + 3)),
        scratch_shapes=scratch,
        compiler_params=pltpu.CompilerParams(
            collective_id=3, has_side_effects=True, vmem_limit_bytes=60 << 20
        ),
        name="front_gather",
    )(*xs, wp, pk, gn)


def add_blocks(dst, srcs):
    rows = dst.shape[0]
    width = dst.shape[1]
    step = 16 if rows % 16 == 0 else rows

    @pl.loop(0, rows // step)
    def _(i):
        at = pl.ds(pl.multiple_of(i * step, step), step)
        total = srcs[0][at, :].astype(F32)
        for s_ref in srcs[1:]:
            total = total + s_ref[at, :].astype(F32)
        dst[at, :] = total.astype(dst.dtype)


def scatter_stages(part, out, ybuf, zbuf, sbuf, qbuf, y_send, y_recv, z_send, z_recv, q_send, q_recv, spacing=1):
    s = lax.axis_index("seq")
    z, y = s // 2, lax.rem(s, 2)
    other = s + 1 - 2 * y
    rows = out.shape[0]
    slabs = rows // SLAB
    np_ = ybuf.shape[1]
    items = [(c, own, False) for c in range(np_, slabs) for own in (True, False)] + [(c, True, True) for c in range(np_)]

    def own_part(zz, yy, c):
        return part.at[pl.ds(pl.multiple_of((zz * 2 + yy) * rows + c * SLAB, SLAB), SLAB), :]

    def y_at(k):
        return jnp.where(z < 2, 3 - k, k)

    def y_copy(c, k):
        zz = y_at(k)
        at = c * 4 + k
        return remote(own_part(zz, 1 - y, c), ybuf.at[zz, c], y_send.at[at], y_recv.at[at], {"seq": other})

    def base(i, zz):
        c, own, crossed = items[i]
        yy = y if own else 1 - y
        refs = [own_part(zz, yy, c)]
        if crossed:
            refs.append(ybuf.at[zz, c])
        return refs

    def z_at(direction, q, i):
        return (direction * 4 + q) * len(items) + i

    def z_copy(direction, h, q, i):
        zz = q if direction == 0 else 3 - q
        refs = base(i, zz)
        src = refs[0] if (h == 0 and len(refs) == 1) else sbuf.at[direction, q - 1, i]
        at = z_at(direction, q, i)
        return remote(
            src, zbuf.at[direction, q - 1, i], z_send.at[at], z_recv.at[at], {"seq": s + 2 if direction == 0 else s - 2}
        )

    def hop(i, h):
        for direction in (0, 1):
            pos = z if direction == 0 else 3 - z

            @pl.when(pos == h)
            def _():
                for q in range(3, h - 1, -1):
                    if h > 0:
                        z_copy(direction, h, q, i).wait_recv()
                    if q > h:
                        zz = q if direction == 0 else 3 - q
                        refs = base(i, zz)
                        if h > 0:
                            refs = refs + [zbuf.at[direction, q - 1, i]]
                        if len(refs) > 1:
                            add_blocks(sbuf.at[direction, q - 1, i], refs)
                        z_copy(direction, h, q, i).start()

    def q_copy(j):
        return remote(qbuf.at[0, j], qbuf.at[1, j], q_send.at[j], q_recv.at[j], {"seq": other})

    def settle(i):
        c, own, crossed = items[i]
        dst = out.at[pl.ds(c * SLAB, SLAB), :] if own else qbuf.at[0, c - np_]
        for low, high in ((True, False), (False, False), (False, True)):
            where = z == 0 if low else (z == 3 if high else jnp.logical_and(z > 0, z < 3))

            @pl.when(where)
            def _():
                refs = base(i, z)
                if not low:
                    refs = refs + [zbuf.at[0, z - 1, i]]
                if not high:
                    refs = refs + [zbuf.at[1, 2 - z, i]]
                add_blocks(dst, refs)

        if not own:
            q_copy(c - np_).start()

    def start():
        for c in range(np_):
            for k in range(4):
                y_copy(c, k).start()

    def y_wait(i):
        c, own, crossed = items[i]
        if crossed:
            for k in range(4):
                y_copy(c, k).wait_recv()

    steps = []
    for tau in range(len(items) + 4 * spacing):
        group = []
        for i in range(len(items)):
            h = tau - i
            if 0 <= h <= 4 * spacing and h % spacing == 0:
                group.append((i, h // spacing))

        def step(group=group):
            for i, h in group:
                if h == 0:
                    y_wait(i)
                if h < 4:
                    hop(i, h)
                else:
                    settle(i)

        steps.append(step)

    def finish():
        for c in range(np_, slabs):
            q_copy(c - np_).wait_recv()
            dst = out.at[pl.ds(c * SLAB, SLAB), :]
            add_blocks(dst, [dst, qbuf.at[1, c - np_]])
        for c in range(np_, slabs):
            q_copy(c - np_).wait_send()
        for c in range(np_):
            for k in range(4):
                y_copy(c, k).wait_send()
        for i in range(len(items)):
            for direction in (0, 1):
                pos = z if direction == 0 else 3 - z
                for h in range(3):

                    @pl.when(pos == h)
                    def _():
                        for q in range(3, h, -1):
                            z_copy(direction, h, q, i).wait_send()

    return start, steps, finish


def scatter_scratch(rows, width, np_):
    slabs = rows // SLAB
    nq = slabs - np_
    count = 2 * nq + np_
    dma = pltpu.SemaphoreType.DMA
    return [
        pltpu.VMEM((4, np_, SLAB, width), BF),
        pltpu.VMEM((2, 3, count, SLAB, width), BF),
        pltpu.VMEM((2, 3, count, SLAB, width), BF),
        pltpu.VMEM((2, nq, SLAB, width), BF),
        dma((4 * np_,)),
        dma((4 * np_,)),
        dma((8 * count,)),
        dma((8 * count,)),
        dma((nq,)),
        dma((nq,)),
    ]


def reduce_stages(src, cbuf, abuf, xbuf, c_send, c_recv, x_send, x_recv, blocks, order, settle):
    d = lax.axis_index("dp")
    cross = lax.rem(d + 2, 4)
    core = d + 1 - 2 * lax.rem(d, 2)
    diag = lax.rem(core + 2, 4)

    def c_copy(kind, b):
        at = kind * blocks + b
        return remote(src(diag if kind else core, order(b)), cbuf.at[kind, b], c_send.at[at], c_recv.at[at], {"dp": core})

    def x_copy(b):
        return remote(abuf.at[b], xbuf.at[b], x_send.at[b], x_recv.at[b], {"dp": cross})

    def start():
        for kind in (1, 0):
            for b in range(blocks):
                c_copy(kind, b).start()

    def first(b):
        c_copy(1, b).wait_recv()
        add_blocks(abuf.at[b], [src(cross, order(b)), cbuf.at[1, b]])
        x_copy(b).start()

    def second(b):
        c_copy(0, b).wait_recv()
        x_copy(b).wait_recv()
        settle(b, [src(d, order(b)), cbuf.at[0, b], xbuf.at[b]])

    def finish():
        for b in range(blocks):
            for kind in (0, 1):
                c_copy(kind, b).wait_send()
            x_copy(b).wait_send()

    return start, first, second, finish


def reduce_scratch(blocks, rows, width):
    dma = pltpu.SemaphoreType.DMA
    return [
        pltpu.VMEM((2, blocks, rows, width), BF),
        pltpu.VMEM((blocks, rows, width), BF),
        pltpu.VMEM((blocks, rows, width), BF),
        dma((2 * blocks,)),
        dma((2 * blocks,)),
        dma((blocks,)),
        dma((blocks,)),
    ]


def tail_kernel(count, n_pack, *refs):
    parts, refs = refs[:count], refs[count:]
    g, refs = refs[0], refs[1:]
    pg, refs = (refs[0], refs[1:]) if n_pack else (None, refs)
    outs, refs = refs[:count], refs[count:]
    gout, refs = refs[0], refs[1:]
    pout, refs = (refs[0], refs[1:]) if n_pack else (None, refs)
    scat = [refs[i * 10 : i * 10 + 10] for i in range(count)]
    refs = refs[10 * count :]
    red, refs = refs[:7], refs[7:]
    packed_red, refs = (refs[:7], refs[7:]) if n_pack else (None, refs)
    fbuf, f_send, f_recv = refs
    s = lax.axis_index("seq")
    d = lax.axis_index("dp")
    n = 8
    peers = [lax.rem(s + k, n) for k in range(1, n)]
    peers_barrier(peers, [lax.rem(d + 2, 4), d + 1 - 2 * lax.rem(d, 2)])

    def order(b):
        return lax.rem(s + b, n)

    def f_copy(b):
        return remote(fbuf.at[b - 1], gout.at[s], f_send.at[b - 1], f_recv.at[b - 1], {"seq": order(b)})

    def f_settle(b, srcs):
        if b == 0:
            add_blocks(gout.at[s], srcs)
        else:
            add_blocks(fbuf.at[b - 1], srcs)
            f_copy(b).start()

    scatters = [scatter_stages(p, o, *sc) for p, o, sc in zip(parts, outs, scat)]
    start, first, second, finish = reduce_stages(lambda dd, b: g.at[dd, b], *red, n, order, f_settle)
    for sc in scatters:
        sc[0]()
    start()
    if n_pack:

        def p_settle(b, srcs):
            add_blocks(pout.at[pl.ds(b * SLAB, SLAB), :], srcs)

        p_start, p_first, p_second, p_finish = reduce_stages(
            lambda dd, b: pg.at[dd, pl.ds(b * SLAB, SLAB), :], *packed_red, n_pack, lambda b: b, p_settle
        )
        p_start()
    blocks = [4, 3, 5, 2, 6, 1, 7, 0]
    todo = []
    for b in blocks:
        todo.append(lambda b=b: first(b))
    if n_pack:
        for b in range(n_pack):
            todo.append(lambda b=b: p_first(b))
    seconds = [lambda b=b: second(b) for b in blocks]
    if n_pack:
        seconds = seconds + [lambda b=b: p_second(b) for b in range(n_pack)]
    steps = [st for group in zip(*[sc[1] for sc in scatters]) for st in group]
    if steps:
        steps.pop(0)()
    for t in todo:
        t()
    while steps or seconds:
        if steps:
            steps.pop(0)()
        if seconds:
            seconds.pop(0)()
    for sc in scatters:
        sc[2]()
    for b in range(1, n):
        f_copy(b).wait()
    finish()
    if n_pack:
        p_finish()


def tail_scatter(parts, g, pg, np_):
    rows, width = parts[0].shape[0] // 8 if parts else 0, parts[0].shape[1] if parts else 0
    count = len(parts)
    n_pack = 0 if pg is None else pg.shape[1] // SLAB
    out_shape = [jax.ShapeDtypeStruct((rows, width), F32)] * count + [jax.ShapeDtypeStruct(g.shape[1:], BF)]
    scratch = []
    for _ in range(count):
        scratch += scatter_scratch(rows, width, np_)
    scratch += reduce_scratch(8, g.shape[2], g.shape[3])
    args = list(parts) + [g]
    if n_pack:
        out_shape.append(jax.ShapeDtypeStruct(pg.shape[1:], F32))
        scratch += reduce_scratch(n_pack, SLAB, pg.shape[2])
        args.append(pg)
    scratch += [pltpu.VMEM((7,) + g.shape[2:], BF), pltpu.SemaphoreType.DMA((7,)), pltpu.SemaphoreType.DMA((7,))]
    return pl.pallas_call(
        functools.partial(tail_kernel, count, n_pack),
        out_shape=tuple(out_shape),
        in_specs=[pl.BlockSpec(memory_space=pltpu.VMEM)] * len(args),
        out_specs=tuple([pl.BlockSpec(memory_space=pltpu.VMEM)] * len(out_shape)),
        scratch_shapes=scratch,
        compiler_params=pltpu.CompilerParams(
            collective_id=4, has_side_effects=True, vmem_limit_bytes=63 << 20
        ),
        name="tail_scatter",
    )(*args)


def silu_slope(values_in):
    sigmoid_value = jax.nn.sigmoid(values_in)
    return sigmoid_value * (1.0 + values_in * (1.0 - sigmoid_value))


def dot(a, b, dims):
    return lax.dot_general(a, b, (dims, ((), ())), preferred_element_type=F32)


def segments(length):
    count = max(1, length // SEGMENT)
    size = length // count
    return [(i * size, (i + 1) * size) for i in range(count)]


def forward_scan(step_size, inner, picked, rate2, shard):
    state = rate2.shape[0]
    carry = jnp.zeros(rate2.shape, F32)
    outs, starts = [], []
    for lo, hi in segments(step_size.shape[0]):
        y, start, carry, *gathered = scan_fwd(
            step_size[lo:hi], inner[lo:hi], picked[:, lo:hi], rate2, carry, RANK, state, shard
        )
        outs.append(y)
        starts.append(start)
    return (outs[0] if len(outs) == 1 else jnp.concatenate(outs, axis=0)), starts, gathered


def backward_scan(step_size, inner, grad_scan, picked, rate2, starts, part):
    state = rate2.shape[0]
    carry = jnp.zeros(rate2.shape, F32)
    parts = []
    total = jnp.zeros(rate2.shape, F32)
    spans = segments(step_size.shape[0])
    for (lo, hi), start in reversed(list(zip(spans, starts))):
        s1, s2, decay, gwr, carry, *summed = scan_bwd(
            step_size[lo:hi], inner[lo:hi], grad_scan[lo:hi], picked[:, lo:hi], rate2, start, carry, RANK, state, part
        )
        total = total + decay
        parts.append((s1, s2, gwr))
    parts = parts[::-1]
    if len(parts) == 1:
        s1, s2, gwr = parts[0]
    else:
        s1, s2, gwr = (jnp.concatenate(p, axis=k) for k, p in zip((0, 0, 1), zip(*parts)))
    return s1, s2, gwr, total, summed


def project_kernel(hide, *refs):
    x_ref, w_ref, gain_ref, conv_ref, sel_ref = refs[:5]
    refs = refs[5:]
    extra_in, refs = refs[:hide], refs[hide:]
    normed_ref, conv_in_ref, gate_ref, out_ref, inner_ref, part_ref = refs[:6]
    refs = refs[6:]
    extra_out, refs = refs[:hide], refs[hide:]
    ext = refs[0]
    turn = pl.program_id(0)
    local = conv_in_ref.shape[1]
    rows = x_ref.shape[1]
    turns = 8
    steps = []
    if hide:
        s = lax.axis_index("seq")
        d = lax.axis_index("dp")
        start, steps, finish = gather_stages(extra_in[0], extra_out[0], *refs[1:5])
        own = pltpu.make_async_copy(extra_in[0], extra_out[0].at[s], refs[5])

    def point(part):
        per = len(steps) / (2.0 * turns - 1)
        for i in range(turns):
            lo, hi = (int(round(per * min(2 * i + part + j, 2 * turns - 1))) for j in (0, 1))
            if hi > lo:

                @pl.when(turn == i)
                def _():
                    for st in steps[lo:hi]:
                        st()

    @pl.when(turn == 0)
    def _():
        ext[0:8, :] = jnp.zeros((8, local), F32)
        if hide:
            peers_barrier([lax.rem(s + k, 8) for k in range(1, 8)], [lax.rem(d + 2, 4), d + 1 - 2 * lax.rem(d, 2)])
            start()
            own.start()

    xf = x_ref[0].astype(F32)
    scale = lax.rsqrt(jnp.mean(xf * xf, axis=1, keepdims=True) + EPS)
    normed = (xf * scale * gain_ref[...]).astype(BF)
    normed_ref[...] = normed
    mixed = jnp.dot(normed, w_ref[...], preferred_element_type=F32).astype(BF)
    conv_in_ref[...] = mixed[:, :local]
    gate_ref[...] = mixed[:, local:]
    ext[8 : 8 + rows, :] = mixed[:, :local].astype(F32)
    point(0)
    conv = conv_ref[KERNEL : KERNEL + 1, :] + jnp.zeros((rows, local), F32)
    for k in range(KERNEL):
        conv = conv + ext[9 - KERNEL + k : 9 - KERNEL + k + rows, :] * conv_ref[k : k + 1, :]
    out_ref[...] = conv
    inner = (conv * jax.nn.sigmoid(conv)).astype(BF)
    inner_ref[...] = inner.astype(F32)
    last = ext[rows : rows + 8, :]
    ext[0:8, :] = last
    part_ref[...] = dot(sel_ref[...], inner, ((0,), (1,))).astype(BF)
    point(1)
    if hide:

        @pl.when(turn == turns - 1)
        def _():
            finish()
            own.wait()


def project(x, in_w, gain, conv_rows, sel_w, shard):
    blocks, rows, width = x.shape
    length = blocks * rows
    local = in_w.shape[1] // 2
    cols = sel_w.shape[1]
    vmem = pl.BlockSpec(memory_space=pltpu.VMEM)
    wide = lambda w: pl.BlockSpec((rows, w), lambda i: (i, 0))
    args = [x, in_w, gain, conv_rows, sel_w]
    in_specs = [pl.BlockSpec((1, rows, width), lambda i: (i, 0, 0))] + [vmem] * 4
    out_shape = [
        jax.ShapeDtypeStruct((length, width), BF),
        jax.ShapeDtypeStruct((length, local), BF),
        jax.ShapeDtypeStruct((length, local), BF),
        jax.ShapeDtypeStruct((length, local), F32),
        jax.ShapeDtypeStruct((length, local), F32),
        jax.ShapeDtypeStruct((cols, length), BF),
    ]
    out_specs = [wide(width), wide(local), wide(local), wide(local), wide(local), pl.BlockSpec((cols, rows), lambda i: (0, i))]
    scratch = [pltpu.VMEM((rows + 8, local), F32)]
    params = dict(vmem_limit_bytes=50 << 20)
    if shard is not None:
        args.append(shard)
        in_specs.append(vmem)
        out_shape.append(jax.ShapeDtypeStruct((8,) + shard.shape, BF))
        out_specs.append(pl.BlockSpec(memory_space=pl.ANY))
        scratch += gather_sems(shard.shape[0]) + [pltpu.SemaphoreType.DMA]
        params.update(collective_id=7, has_side_effects=True)
    return pl.pallas_call(
        functools.partial(project_kernel, 0 if shard is None else 1),
        grid=(blocks,),
        out_shape=tuple(out_shape),
        in_specs=in_specs,
        out_specs=tuple(out_specs),
        scratch_shapes=scratch,
        compiler_params=pltpu.CompilerParams(**params),
        name="project",
    )(*args)


def shards(
    block_input,
    norm_gain,
    in_weight,
    conv_weight,
    conv_bias,
    select_weight,
    step_weight,
    step_bias,
    decay_log,
    skip_gain,
    out_weight,
    output_grad,
):
    n_dp, n_seq = lax.axis_size("dp"), lax.axis_size("seq")
    token_rows = block_input[0]
    upstream_rows = output_grad[0]
    width = token_rows.shape[1]
    d_rows = in_weight.shape[0]
    e_rows = out_weight.shape[0]
    local = n_dp * e_rows

    own = token_rows.astype(F32)
    own_scale = lax.rsqrt(jnp.mean(own * own, axis=1, keepdims=True) + EPS)
    pieces = in_weight
    pieces = pieces.reshape(d_rows, 2, n_dp, n_seq, e_rows).transpose(3, 0, 1, 2, 4).reshape(n_seq, d_rows, 2 * local)

    smalls = [select_weight, step_weight, decay_log, conv_weight, conv_bias[:, None], step_bias[:, None], skip_gain[:, None]]
    used = sum(s.shape[1] for s in smalls)
    pad = -used % 128
    packed = jnp.concatenate([out_weight] + smalls + [jnp.zeros((e_rows, pad), BF)], axis=1)
    kernels = (n_dp, n_seq) == (4, 8)
    hide = kernels and HIDE
    if kernels:
        gain_tile = jnp.broadcast_to(jnp.pad(norm_gain.astype(F32), (0, 128 - d_rows))[None], (8, 128))
        *gathered, in_w, packed, gains = front_gather(
            [token_rows] if hide else [token_rows, upstream_rows], pieces, packed, gain_tile
        )
        x = gathered[0]
        packed = packed.reshape(local, packed.shape[2])
        gain = gains[:, :, 0, :d_rows].reshape(width)
    else:
        x = lax.all_gather(token_rows, "seq")
        gathered = [x, lax.all_gather(upstream_rows, "seq")]
        in_w = lax.all_gather(lax.all_to_all(pieces, "seq", 0, 0), "dp")
        packed = lax.all_gather(packed, "dp", axis=0, tiled=True)
        gain = lax.all_gather(norm_gain, ("dp", "seq"), axis=0, tiled=True).astype(F32)
    length = n_seq * token_rows.shape[0]
    in_w = in_w.reshape(width, 2 * local)
    cuts = []
    begin = 0
    for s in [out_weight] + smalls:
        cuts.append((begin, begin + s.shape[1]))
        begin += s.shape[1]
    out_w, sel_w, step_w, dec_w, conv_w, conv_b, step_b, skip = (packed[:, a:b] for a, b in cuts)
    conv_taps = conv_w.astype(F32).T
    conv_b, step_b, skip = (v[:, 0].astype(F32) for v in (conv_b, step_b, skip))
    decay_rate = -jnp.exp(dec_w.astype(F32).T)
    rate2 = decay_rate * (1.0 / LN2)

    conv_rows = jnp.concatenate([conv_taps, conv_b[None], jnp.zeros((8 - KERNEL - 1, local), F32)], axis=0)
    half = width // 2
    normed, conv_in, gate_in, conv_out, inner_f, part, *early = project(
        x, in_w, gain[None], conv_rows, sel_w, upstream_rows[:, :half] if hide else None
    )
    gate_in = gate_in.astype(F32)
    inner = inner_f.astype(BF)
    padded = jnp.concatenate([jnp.zeros((KERNEL - 1, local), BF), conv_in], axis=0).astype(F32)
    picked = sum_over_seq(part, n_seq, "sum_picked", 1)
    step_in = picked[:RANK]
    step_raw = dot(step_in, step_w, ((0,), (1,))) + step_b
    step_size = jax.nn.softplus(step_raw)
    scanned, starts, more = forward_scan(step_size, inner_f, picked, rate2, upstream_rows[:, half:] if hide else None)
    mamba_out = scanned + skip * inner_f
    gate_act = jax.nn.silu(gate_in)
    gated_out = (mamba_out * gate_act).astype(BF)
    out_part = dot(gated_out, out_w, ((1,), (0,))).astype(BF)

    upstream = early + more if hide else [gathered[1]]
    upstream = [u.reshape(length, -1) for u in upstream]
    lows = [i * upstream[0].shape[1] for i in range(len(upstream))]
    grad_gated = sum(dot(u, out_w[:, lo : lo + u.shape[1]], ((1,), (1,))) for u, lo in zip(upstream, lows))
    grad_out_w = [dot(gated_out, u, ((0,), (0,))) for u in upstream]
    grad_scan = grad_gated * gate_act
    grad_gate = grad_gated * mamba_out * silu_slope(gate_in)
    grad_skip = jnp.sum(grad_scan * inner_f, axis=0)
    s1, s2, grad_wr, grad_decay, more = backward_scan(
        step_size, inner_f, grad_scan, picked, rate2, starts, out_part if hide else None
    )
    grad_raw_f = (s1 * LN2 + inner_f * s2) * jax.nn.sigmoid(step_raw)
    grad_step_b = jnp.sum(grad_raw_f, axis=0)
    grad_raw = grad_raw_f.astype(BF)
    grad_step_w = dot(grad_raw, step_in, ((0,), (1,)))
    part = jnp.concatenate([dot(step_w, grad_raw, ((0,), (1,))), grad_wr], axis=0).astype(BF)
    grad_picked = sum_over_seq(part, n_seq, "sum_grad_picked", 2)
    grad_sel = dot(inner, grad_picked, ((0,), (1,)))
    grad_inner = step_size * s2 + grad_scan * skip + dot(grad_picked, sel_w, ((0,), (1,)))
    grad_conv = grad_inner * silu_slope(conv_out)
    grad_conv_b = jnp.sum(grad_conv, axis=0)
    grad_taps = [jnp.sum(grad_conv * padded[k : k + length], axis=0) for k in range(KERNEL)]
    extended = jnp.concatenate([grad_conv, jnp.zeros((KERNEL - 1, local), F32)], axis=0)
    grad_conv_in = jnp.zeros((length, local), F32)
    for k in range(KERNEL):
        grad_conv_in = grad_conv_in + extended[KERNEL - 1 - k : KERNEL - 1 - k + length] * conv_taps[k]
    grad_mixed = jnp.concatenate([grad_conv_in, grad_gate], axis=1).astype(BF)
    grad_in_w = dot(normed, grad_mixed, ((0,), (0,)))
    grad_normed = dot(grad_mixed, in_w, ((1,), (1,)))

    small_grads = [grad_sel, grad_step_w, (grad_decay * decay_rate).T, jnp.stack(grad_taps, axis=1), grad_conv_b[:, None], grad_step_b[:, None], grad_skip[:, None]]
    packed_grad = jnp.concatenate(grad_out_w + small_grads + [jnp.zeros((local, pad), F32)], axis=1).astype(BF)
    grad_in_w = grad_in_w.astype(BF)
    grad_normed = grad_normed.astype(BF)
    if kernels:
        parts = [grad_normed] if hide else [grad_normed, out_part]
        *summed, grad_in_all, packed_grad = tail_scatter(
            parts,
            grad_in_w.reshape(n_dp, n_seq, d_rows, 2 * local),
            packed_grad.reshape(n_dp, e_rows, packed_grad.shape[1]),
            BNP,
        )
        grad_normed = summed[0]
        out_rows = more[0] if hide else summed[1]
    else:
        packed_grad = lax.psum_scatter(packed_grad, "dp", scatter_dimension=0, tiled=True).astype(F32)
        grad_in_all = lax.psum_scatter(grad_in_w, "dp", scatter_dimension=0, tiled=True)
        grad_in_all = lax.all_to_all(grad_in_all, "seq", split_axis=0, concat_axis=0, tiled=True)
        grad_in_all = grad_in_all.reshape(n_seq, d_rows, 2 * local)
        grad_normed = lax.psum_scatter(grad_normed, "seq", scatter_dimension=0, tiled=True).astype(F32)
        out_rows = lax.psum_scatter(out_part, "seq", scatter_dimension=0, tiled=True)
    layer_out = (own + out_rows.astype(F32)).astype(BF)
    g_out, g_sel, g_step, g_dec, g_conv, g_cb, g_sb, g_skip = (packed_grad[:, a:b] for a, b in cuts)
    g_in = (
        grad_in_all.reshape(n_seq, d_rows, 2, n_dp, e_rows)
        .transpose(1, 2, 3, 0, 4)
        .reshape(in_weight.shape)
        .astype(F32)
    )
    g_gain = jnp.sum(g_in * in_weight.astype(F32), axis=1) / norm_gain.astype(F32)

    scaled = grad_normed * gain
    grad_rows = own_scale * scaled - own * (own_scale * own_scale * own_scale) * jnp.mean(scaled * own, axis=1, keepdims=True)
    input_grad = (upstream_rows.astype(F32) + grad_rows).astype(BF)
    return (
        layer_out[None],
        input_grad[None],
        g_gain,
        g_in,
        g_conv,
        g_cb[:, 0],
        g_sel,
        g_step,
        g_sb[:, 0],
        g_dec,
        g_skip[:, 0],
        g_out,
    )


def solution(mesh):
    rows = P(("dp", "seq"))
    both = P(("dp", "seq"), None)
    acts = P("dp", "seq", None)
    return jax.shard_map(
        shards,
        mesh=mesh,
        in_specs=(acts, rows, both, both, rows, both, both, rows, both, rows, both, acts),
        out_specs=(acts, acts, rows, both, both, rows, both, both, rows, both, rows, both),
        check_vma=False,
    )
```
